32 devices in a mesh: prow: 4 (over y, core), pcol: 8 (over z, x).
Axes of the slice: x: 2, y: 2, z: 4, core: 2. Of those that a mesh axis runs over, the one named last changes fastest.
Arguments:
- vectors: bfloat16 [512, 120064], P('pcol', 'prow'), may hold values from -6 to 6
- reflectors: bfloat16 [2, 256, 120064], P(None, 'pcol', 'prow'), may hold values from -6 to 6
- panel_factor: float32 [2, 256, 256], replicated, as said below
Outputs:
- band_vectors: bfloat16 [8, 64, 120064], P('pcol', 'prow')
The draws below stay inside these ranges and needn't reach their ends.
Inputs may be any that keep to these rules, and one draw needn't show every extreme that they name: `panel_factor`: upper triangular: zero below the diagonal; diagonal entries between 1 / 120064 and 3 / 120064.
All inputs are finite; a program needn't handle non-finite values.
Results may differ from the reference program's by a relative error of at most 0.0095.
Values may be sent and summed in bfloat16 or wider, within the bound.
A program may use at most 192 MiB of HBM per device.

```python
import jax
import jax.numpy as jnp
from jax import lax

ORDER = 120064
PANEL = 256
PANELS = 2
COLS_DEV = 64
NEV = 512
N_PCOL = 8


def draw_panel_factor(key, part):
    first_key, second_key = jax.random.split(jax.random.fold_in(key, 7))
    shape = (PANELS, PANEL, PANEL)
    upper_part = jax.random.normal(first_key, shape, jnp.float32) * (0.6 / ORDER)
    diag_part = jax.random.uniform(second_key, (PANELS, PANEL), jnp.float32, 1.0, 3.0) / ORDER
    row_ids = lax.broadcasted_iota(jnp.int32, shape, 1)
    col_ids = lax.broadcasted_iota(jnp.int32, shape, 2)
    result = jnp.where(col_ids > row_ids, upper_part, 0.0)
    result = result + jnp.where(col_ids == row_ids, diag_part[:, :, None], 0.0)
    return result.astype(jnp.float32)


def shard_levels(own_key, dims, pieces, low, top_value):
    factor_of = 1.0
    for position, blocks in pieces:
        steps = jax.random.uniform(jax.random.fold_in(jax.random.fold_in(own_key, 6), position), (blocks,), jnp.float32, low / len(pieces), top_value / len(pieces))
        factor_of = factor_of * jnp.repeat(jnp.exp(steps), dims[position] // blocks).reshape((-1,) + (1,) * (len(dims) - 1 - position))
    return factor_of


def scatter_about(rng, shape, deviation, most, cuts=(), dtype=jnp.bfloat16):
    entries = deviation * jax.random.normal(rng, shape, jnp.float32)
    if cuts:
        entries = entries * shard_levels(rng, shape, cuts, -0.22, 0.18)
    return jnp.clip(entries, -most, most).astype(dtype)


def setup_inputs(seed: int = 0) -> dict:
    streams_of = jax.random.split(jax.random.key(seed), 4)
    vectors = scatter_about(streams_of[0], (NEV, ORDER), 1.0, 6.0, ((0, 8), (1, 4)))
    reflectors = scatter_about(streams_of[1], (PANELS, PANEL, ORDER), 1.0, 6.0, ((1, 8), (2, 4)))
    panel_factor = draw_panel_factor(jax.random.fold_in(streams_of[3], 71), 0)
    return dict(vectors=vectors, reflectors=reflectors, panel_factor=panel_factor)


def apply_panel(current, panel, factor):
    projected = lax.dot_general(current, panel, (((1,), (1,)), ((), ())), preferred_element_type=jnp.float32)
    scaled = lax.dot_general(projected, factor, (((1,), (1,)), ((), ())), precision=lax.Precision.HIGHEST, preferred_element_type=jnp.float32).astype(jnp.bfloat16)
    updated = current.astype(jnp.float32) - jnp.dot(scaled, panel, preferred_element_type=jnp.float32)
    return updated.astype(jnp.bfloat16)


def reference(vectors, reflectors, panel_factor):
    current = vectors
    for number in range(PANELS):
        current = apply_panel(current, reflectors[number], panel_factor[number])
    return current.reshape(N_PCOL, COLS_DEV, ORDER)
```

```python
import functools

import jax
import jax.numpy as jnp
from jax import lax
from jax.experimental import pallas as pl
from jax.experimental.pallas import tpu as pltpu
from jax.sharding import PartitionSpec as P

MESH = pl.DeviceIdType.MESH
LANES = 128
SPLIT = 4
F32, BF16 = jnp.float32, jnp.bfloat16
NT = (((1,), (1,)), ((), ()))


def flip(index, bit):
    return index + bit - 2 * bit * lax.rem(lax.div(index, bit), 2)


def flipped(index, mask):
    bit = 1
    while bit <= mask:
        if mask & bit:
            index = flip(index, bit)
        bit *= 2
    return index


def kernel(
    n_row, n_col, columns, plan,
    v_ref, w_ref, vt_ref, wt_ref, t_ref, o_ref,
    v_s, w_s, v_mid, w_mid, v_tail, w_tail, part, rs_send, rs_recv, ag, s_s, stage,
    vx_send, wx_send, v_send, w_send, v_recv, w_recv, m_recv,
    r_send, r_recv, g_send, g_recv, o_send, o_recv, l_sem,
):
    site, main, rest, pieces, sums_at, out_blocks, n_block = plan
    me_r, me_c = lax.axis_index("prow"), lax.axis_index("pcol")
    me_a, me_b = lax.rem(me_c, SPLIT), lax.div(me_c, SPLIT)
    halves, group = n_col // SPLIT, SPLIT * n_row
    me_g = me_a * n_row + me_r
    rows = SPLIT * v_s.shape[1]
    panel = w_s.shape[1] * w_s.shape[2]
    own = v_s.shape[1] // n_row
    side_c, side_a = flip(me_c, 1), flip(me_a, 1)
    far_a = flip(me_a, 2)
    others = [lax.rem(me_b + k, halves) for k in range(1, halves)]

    def turns(mask):
        a, r = mask // n_row, mask % n_row
        first = 0 if a & 2 else 1 if a & 1 else 2 if r > 1 else 3
        size = -(bool(a & 1) * 2 + (r > 1)) if first == 0 else (r > 1)
        return first, size, mask

    masks = sorted(range(1, group), key=turns)

    def partner(mask):
        a, r = flipped(me_a, mask // n_row), flipped(me_r, mask % n_row)
        return a * n_row + r, r, me_b * SPLIT + a

    partners = [partner(mask) for mask in masks]

    barrier = pltpu.get_barrier_semaphore()
    for _, r, c in partners:
        pl.semaphore_signal(barrier, device_id={"prow": r, "pcol": c}, device_id_type=MESH)
    for b in others:
        for a in (me_a, far_a):
            pl.semaphore_signal(
                barrier, device_id={"prow": me_r, "pcol": b * SPLIT + a}, device_id_type=MESH
            )
    pl.semaphore_wait(barrier, len(partners) + 2 * len(others))

    def remote(src, dst, send, recv, r, c):
        return pltpu.make_async_remote_copy(
            src_ref=src, dst_ref=dst, send_sem=send, recv_sem=recv,
            device_id={"prow": r, "pcol": c}, device_id_type=MESH,
        )

    sends = []

    def start(copies, last):
        if len(copies) == 1:
            copies[0].start()
        else:
            pl.when(last)(copies[1].start)
            pl.when(jnp.logical_not(last))(copies[0].start)
        return copies[-1]

    def sources(full, tail, q, at, stop):
        cols = pl.ds(pl.multiple_of(q * site + at, LANES), stop - at)
        found = [full.at[..., cols]]
        if at == main:
            found.append(tail)
        return found

    def send(full, tail, q, number, dst, sent, come, c):
        at, stop = pieces[number]
        copies = [
            remote(src, dst, sent, come, me_r, c) for src in sources(full, tail, q, at, stop)
        ]
        sends.append(start(copies, q == SPLIT - 1))

    def keep(full, tail, q, number, dst, sem):
        at, stop = pieces[number]
        copies = [pltpu.make_async_copy(src, dst, sem) for src in sources(full, tail, q, at, stop)]
        return start(copies, q == SPLIT - 1)

    def cols_of(number):
        at, stop = pieces[number]
        return pl.ds(at, stop - at)

    def along(number, v_from, w_here, w_there, a, c, send_at):
        cols, n = cols_of(number), send_at
        for b in others:
            w_here(number, b * SPLIT + me_a, w_s.at[:, c, :, cols], w_send.at[number, n], w_recv.at[number, c])
            n += 1
            w_there(number, b * SPLIT + far_a, w_s.at[:, c, :, cols], w_send.at[number, n], w_recv.at[number, c])
            n += 1
        to = me_b * SPLIT + far_a
        v_from(number, to, v_s.at[a, :, cols], v_send.at[number, send_at and 1], v_recv.at[number, a])
        w_there(number, to, w_s.at[:, c, :, cols], w_send.at[number, n], w_recv.at[number, c])

    v_tail[...] = jnp.zeros_like(v_tail)
    w_tail[...] = jnp.zeros_like(w_tail)
    if rest:
        v_tail[:, :rest] = vt_ref[:, :rest]
        w_tail[:, :, :rest] = wt_ref[:, :, :rest]
    width = v_s.shape[2]
    if width > site:
        v_s[:, :, site:] = jnp.zeros((SPLIT, v_s.shape[1], width - site), BF16)
        w_s[:, :, :, site:] = jnp.zeros((2, n_col, w_s.shape[2], width - site), BF16)
    part[...] = jnp.zeros_like(part)

    def from_v(q):
        return lambda number, c, dst, sent, come: send(v_ref, v_tail, q, number, dst, sent, come, c)

    def from_w(q):
        return lambda number, c, dst, sent, come: send(w_ref, w_tail, q, number, dst, sent, come, c)

    side_far = flip(side_a, 2)
    local = []
    for number in range(len(pieces)):
        cols = cols_of(number)
        w_first = from_w(side_far)
        w_first(number, side_c, w_mid.at[:, :, cols], wx_send.at[number, 0], m_recv.at[number, 0])
        from_v(side_far)(number, side_c, v_mid.at[:, cols], vx_send.at[number, 0], m_recv.at[number, 1])
        from_w(side_a)(
            number, side_c, w_s.at[:, me_c, :, cols], wx_send.at[number, 1], w_recv.at[number, me_c]
        )
        from_v(side_a)(
            number, side_c, v_s.at[me_a, :, cols], vx_send.at[number, 1], v_recv.at[number, me_a]
        )
        along(number, from_v(far_a), from_w(me_a), from_w(far_a), me_a, me_c, 0)
        local.append((
            keep(v_ref, v_tail, me_a, number, v_s.at[me_a, :, cols], l_sem.at[number, 0]),
            keep(w_ref, w_tail, me_a, number, w_s.at[:, me_c, :, cols], l_sem.at[number, 1]),
        ))

    def come(dst, sem):
        remote(dst, dst, sem, sem, me_r, side_c).wait_recv()

    def passed_on(src):
        def start_copy(number, c, dst, sent, recv):
            copy = remote(src(number), dst, sent, recv, me_r, c)
            copy.start()
            sends.append(copy)
        return start_copy

    for number in range(len(pieces)):
        cols = cols_of(number)
        come(w_mid.at[:, :, cols], m_recv.at[number, 0])
        come(v_mid.at[:, cols], m_recv.at[number, 1])
        come(w_s.at[:, side_c, :, cols], w_recv.at[number, side_c])
        come(v_s.at[side_a, :, cols], v_recv.at[number, side_a])
        along(
            number,
            passed_on(lambda n: v_mid.at[:, cols_of(n)]),
            passed_on(lambda n: w_s.at[:, side_c, :, cols_of(n)]),
            passed_on(lambda n: w_mid.at[:, :, cols_of(n)]),
            side_a, side_c, 2 * halves - 1,
        )

    def panel_of(p, cols):
        block = w_s[p, :, :, cols]
        if w_s.shape[2] % 16:
            block = block.astype(F32)
        return block.reshape(panel, block.shape[-1]).astype(BF16)

    def products(at, stop):
        cols = pl.ds(at, stop - at)
        v = v_s[:, :, cols].reshape(rows, stop - at)
        first, second = panel_of(0, cols), panel_of(1, cols)
        part[:, :panel] += lax.dot_general(v, first, NT, preferred_element_type=F32)
        part[:, panel:2 * panel] += lax.dot_general(v, second, NT, preferred_element_type=F32)
        part[:, 2 * panel:] += lax.dot_general(first, second, NT, preferred_element_type=F32)

    for number in range(len(pieces)):
        cols = cols_of(number)
        for copy in local[number]:
            copy.wait()
        for a in (far_a, side_far):
            come(v_s.at[a, :, cols], v_recv.at[number, a])
        for b in [me_b] + others:
            for a in (me_a, side_a, far_a, side_far):
                if b is me_b and (a is me_a or a is side_a):
                    continue
                c = b * SPLIT + a
                come(w_s.at[:, c, :, cols], w_recv.at[number, c])
        products(*sums_at[number])

    rs_send[...] = part[...].astype(BF16).reshape(rs_send.shape)
    for g, r, c in partners:
        copy = remote(rs_send.at[g], rs_recv.at[me_g], r_send.at[g], r_recv.at[me_g], r, c)
        copy.start()
        sends.append(copy)
    total = rs_send[me_g].astype(F32)
    for g, r, c in reversed(partners):
        remote(rs_send.at[g], rs_recv.at[g], r_send.at[g], r_recv.at[g], r, c).wait_recv()
        total += rs_recv[g].astype(F32)
    ag[me_g] = total.astype(BF16)
    for g, r, c in partners:
        copy = remote(ag.at[me_g], ag.at[me_g], g_send.at[g], g_recv.at[me_g], r, c)
        copy.start()
        sends.append(copy)
    for g, r, c in partners:
        remote(ag.at[me_g], ag.at[g], g_send.at[g], g_recv.at[g], r, c).wait_recv()

    sums = ag[...].reshape(rows, 3 * panel)
    high = lax.Precision.HIGHEST
    s1 = lax.dot_general(
        sums[:, :panel].astype(F32), t_ref[0], NT, precision=high, preferred_element_type=F32
    ).astype(BF16)
    p2 = sums[:, panel:2 * panel].astype(F32) - jnp.dot(
        s1, sums[:, 2 * panel:], preferred_element_type=F32
    )
    s2 = lax.dot_general(p2, t_ref[1], NT, precision=high, preferred_element_type=F32).astype(BF16)
    s_s[0] = s1
    s_s[1] = s2

    def piece(a, r, at, size):
        return v_s.at[a, pl.ds(pl.multiple_of(r * own, own), own), pl.ds(at, size)]

    def landing(a, r, at, size):
        return stage.at[r, :, pl.ds(pl.multiple_of(a * site + at, LANES), size)]

    for j, (at, stop) in enumerate(out_blocks):

        @pl.loop(at // n_block, stop // n_block)
        def _(i):
            cols = pl.ds(pl.multiple_of(i * n_block, n_block), n_block)
            v = v_s[:, :, cols].reshape(rows, n_block).astype(F32)
            v = v - jnp.dot(s_s[0], panel_of(0, cols), preferred_element_type=F32)
            v = v - jnp.dot(s_s[1], panel_of(1, cols), preferred_element_type=F32)
            v_s[:, :, cols] = v.astype(BF16).reshape(SPLIT, rows // SPLIT, n_block)

        size = min(stop, site) - at
        for g, r, c in partners:
            a = lax.div(g, n_row)
            copy = remote(
                piece(a, r, at, size), landing(me_a, me_r, at, size),
                o_send.at[g, j], o_recv.at[me_g, j], r, c,
            )
            copy.start()
            sends.append(copy)

    for j, (at, stop) in enumerate(out_blocks):
        size = min(stop, site) - at
        stage[me_r, :, pl.ds(pl.multiple_of(me_a * site + at, LANES), size)] = v_s[
            me_a, pl.ds(pl.multiple_of(me_r * own, own), own), pl.ds(at, size)
        ]
        for g, r, c in partners:
            a = lax.div(g, n_row)
            remote(
                piece(a, r, at, size), landing(a, r, at, size), o_send.at[g, j], o_recv.at[g, j], r, c
            ).wait_recv()
        for r in range(n_row):
            for a in range(SPLIT):
                begin, end = a * site + at, min(a * site + at + size, columns)
                if end > begin:
                    o_ref[:, r * columns + begin:r * columns + end] = stage[r, :, begin:end]
    for copy in sends:
        copy.wait_send()


def body(n_row, n_col, vectors, reflectors, panel_factor):
    own_rows, columns = vectors.shape
    part_rows, panel = reflectors.shape[1], panel_factor.shape[1]
    halves, group, rows = n_col // SPLIT, SPLIT * n_row, SPLIT * own_rows
    site = -(-columns // (SPLIT * LANES)) * LANES
    last = columns - (SPLIT - 1) * site
    main, rest = last // LANES * LANES, last % LANES
    n_block = 2 * LANES
    width = -(-site // n_block) * n_block
    step = -(-main // (4 * n_block)) * n_block
    cuts = list(range(0, main, step)) + [main]
    even = main // n_block * n_block
    pieces = tuple(zip(cuts[:-1], cuts[1:])) + ((main, site),)
    sums_at = tuple((s, min(e, even)) for s, e in pieces[:-1]) + ((even, width),)
    marks = [0, 2 * n_block]
    blocks = width // n_block
    marks += [n_block * (2 + (blocks - 2) * k // 6) for k in range(1, 7)]
    out_blocks = tuple(zip(marks[:-1], marks[1:]))
    edge = min(((SPLIT - 1) * site + main) // LANES, -(-columns // LANES) - 1)
    count, hops = len(pieces), 2 * (2 * halves - 1)
    dma = pltpu.SemaphoreType.DMA
    plan = (site, main, rest, pieces, sums_at, out_blocks, n_block)
    whole = pl.pallas_call(
        functools.partial(kernel, n_row, n_col, columns, plan),
        grid=(1,),
        out_shape=jax.ShapeDtypeStruct((own_rows // n_row, n_row * columns), BF16),
        in_specs=[
            pl.BlockSpec(memory_space=pl.ANY),
            pl.BlockSpec(memory_space=pl.ANY),
            pl.BlockSpec((own_rows, LANES), lambda i: (0, edge)),
            pl.BlockSpec((2, part_rows, LANES), lambda i: (0, 0, edge)),
            pl.BlockSpec(panel_factor.shape, lambda i: (0, 0, 0)),
        ],
        out_specs=pl.BlockSpec(memory_space=pltpu.VMEM),
        scratch_shapes=[
            pltpu.VMEM((SPLIT, own_rows, width), BF16),
            pltpu.VMEM((2, n_col, part_rows, width), BF16),
            pltpu.VMEM((own_rows, site), BF16),
            pltpu.VMEM((2, part_rows, site), BF16),
            pltpu.VMEM((own_rows, site - main), BF16),
            pltpu.VMEM((2, part_rows, site - main), BF16),
            pltpu.VMEM((rows, 3 * panel), F32),
            pltpu.VMEM((group, rows // group, 3 * panel), BF16),
            pltpu.VMEM((group, rows // group, 3 * panel), BF16),
            pltpu.VMEM((group, rows // group, 3 * panel), BF16),
            pltpu.VMEM((2, rows, panel), BF16),
            pltpu.VMEM((n_row, own_rows // n_row, SPLIT * site), BF16),
            dma((count, 2)), dma((count, 2)), dma((count, 2)), dma((count, hops)),
            dma((count, SPLIT)), dma((count, n_col)), dma((count, 2)),
            dma((group,)), dma((group,)), dma((group,)), dma((group,)),
            dma((group, len(out_blocks))), dma((group, len(out_blocks))), dma((count, 2)),
        ],
        compiler_params=pltpu.CompilerParams(
            has_side_effects=True, collective_id=0, vmem_limit_bytes=48 * 1024 * 1024
        ),
        name="panels",
    )(vectors, reflectors, vectors, reflectors, panel_factor)
    return whole[None]


def solution(mesh):
    placed = (P("pcol", "prow"), P(None, "pcol", "prow"), P())
    return jax.shard_map(
        functools.partial(body, mesh.shape["prow"], mesh.shape["pcol"]),
        mesh=mesh, in_specs=placed, out_specs=P("pcol", "prow", None), check_vma=False,
    )
```

```python
import functools

import jax
import jax.numpy as jnp
from jax import lax
from jax.experimental import pallas as pl
from jax.experimental.pallas import tpu as pltpu
from jax.sharding import PartitionSpec as P

MESH = pl.DeviceIdType.MESH
LANES = 128
SPLIT = 4
F32, BF16 = jnp.float32, jnp.bfloat16
NT = (((1,), (1,)), ((), ()))


def flip(index, bit):
    return index + bit - 2 * bit * lax.rem(lax.div(index, bit), 2)


def flipped(index, mask):
    bit = 1
    while bit <= mask:
        if mask & bit:
            index = flip(index, bit)
        bit *= 2
    return index


def kernel(
    n_row, n_col, columns, plan,
    v_ref, w_ref, vt_ref, wt_ref, t_ref, o_ref,
    v_s, w_s, v_mid, w_mid, v_tail, w_tail, t_s, part, rs_send, rs_recv, ag, s_s, stage,
    v_send, w_send, v_recv, w_recv, v_side, w_side, r_send, r_recv, g_send, g_recv,
    o_send, o_recv, l_sem, t_sem,
):
    site, main, rest, pieces, sums_at, out_blocks, n_block = plan
    me_r, me_c = lax.axis_index("prow"), lax.axis_index("pcol")
    me_a, me_b = lax.rem(me_c, SPLIT), lax.div(me_c, SPLIT)
    halves, group = n_col // SPLIT, SPLIT * n_row
    me_g = me_a * n_row + me_r
    rows = SPLIT * v_s.shape[1]
    panel = w_s.shape[1] * w_s.shape[2]
    own = v_s.shape[1] // n_row
    side_c, side_a = flip(me_c, 1), flip(me_a, 1)
    far_a, side_far = flip(me_a, 2), flip(side_a, 2)
    others = [lax.rem(me_b + k, halves) for k in range(1, halves)]

    def turns(mask):
        a, r = mask // n_row, mask % n_row
        first = 0 if a & 2 else 1 if a & 1 else 2 if r > 1 else 3
        size = -(bool(a & 1) * 2 + (r > 1)) if first == 0 else (r > 1)
        return first, size, mask

    masks = sorted(range(1, group), key=turns)

    def partner(mask):
        a, r = flipped(me_a, mask // n_row), flipped(me_r, mask % n_row)
        return a * n_row + r, r, me_b * SPLIT + a

    partners = [partner(mask) for mask in masks]

    barrier = pltpu.get_barrier_semaphore()
    for _, r, c in partners:
        pl.semaphore_signal(barrier, device_id={"prow": r, "pcol": c}, device_id_type=MESH)
    for b in others:
        for a in (me_a, far_a):
            pl.semaphore_signal(
                barrier, device_id={"prow": me_r, "pcol": b * SPLIT + a}, device_id_type=MESH
            )

    def remote(src, dst, send, recv, r, c):
        return pltpu.make_async_remote_copy(
            src_ref=src, dst_ref=dst, send_sem=send, recv_sem=recv,
            device_id={"prow": r, "pcol": c}, device_id_type=MESH,
        )

    def cols_of(number):
        at, stop = pieces[number]
        return pl.ds(at, stop - at)

    def start(make, full, tail, q, number):
        at, stop = pieces[number]
        copy = make(full.at[..., pl.ds(pl.multiple_of(q * site + at, LANES), stop - at)])
        if at == main:
            pl.when(q == SPLIT - 1)(make(tail).start)
            pl.when(q != SPLIT - 1)(copy.start)
        else:
            copy.start()

    def send(full, tail, q, dst, sent, come):
        def start_copy(number, c):
            start(
                lambda src: remote(src, dst(number), sent, come.at[number], me_r, c),
                full, tail, q, number,
            )
        return start_copy

    def pass_on(src, dst, sent, come):
        def start_copy(number, c):
            remote(src(number), dst(number), sent, come.at[number], me_r, c).start()
        return start_copy

    def v_slot(a):
        return lambda number: v_s.at[a, :, cols_of(number)]

    def w_slot(c):
        return lambda number: w_s.at[:, c, :, cols_of(number)]

    def v_half(number):
        return v_mid.at[:, cols_of(number)]

    def w_half(number):
        return w_mid.at[:, :, cols_of(number)]

    def along(number, v_there, w_here, w_there):
        for b in others:
            w_here(number, b * SPLIT + me_a)
            w_there(number, b * SPLIT + far_a)
        v_there(number, me_b * SPLIT + far_a)
        w_there(number, me_b * SPLIT + far_a)

    def wait(ref, sem):
        pltpu.make_async_copy(ref, ref, sem).wait()

    keep_t = pltpu.make_async_copy(t_ref, t_s, t_sem)
    keep_t.start()
    v_tail[...] = jnp.zeros_like(v_tail)
    w_tail[...] = jnp.zeros_like(w_tail)
    if rest:
        v_tail[:, :rest] = vt_ref[:, :rest]
        w_tail[:, :, :rest] = wt_ref[:, :, :rest]
    width = v_s.shape[2]
    if width > site:
        v_s[:, :, site:] = jnp.zeros((SPLIT, v_s.shape[1], width - site), BF16)
        w_s[:, :, :, site:] = jnp.zeros((2, n_col, w_s.shape[2], width - site), BF16)
    part[...] = jnp.zeros_like(part)
    pl.semaphore_wait(barrier, len(partners) + 2 * len(others))

    v_own, w_own = v_slot(me_a), w_slot(me_c)
    v_to = send(v_ref, v_tail, far_a, v_own, v_send, v_recv)
    w_stay = send(w_ref, w_tail, me_a, w_own, w_send, w_recv)
    w_to = send(w_ref, w_tail, far_a, w_own, w_send, w_recv)
    to_side = [
        send(w_ref, w_tail, side_far, w_half, w_send, w_side),
        send(v_ref, v_tail, side_far, v_half, v_send, v_side),
        send(w_ref, w_tail, side_a, w_own, w_send, w_side),
        send(v_ref, v_tail, side_a, v_own, v_send, v_side),
    ]
    for number in range(len(pieces)):
        along(number, v_to, w_stay, w_to)
        for copy in to_side:
            copy(number, side_c)
    for number in range(len(pieces)):
        for k, (full, tail, slot) in enumerate(((v_ref, v_tail, v_own), (w_ref, w_tail, w_own))):
            start(
                lambda src: pltpu.make_async_copy(src, slot(number), l_sem.at[number, k]),
                full, tail, me_a, number,
            )

    v_on = pass_on(v_half, v_slot(side_a), v_send, v_recv)
    w_stay_on = pass_on(w_slot(side_c), w_slot(side_c), w_send, w_recv)
    w_on = pass_on(w_half, w_slot(side_c), w_send, w_recv)
    for number in range(len(pieces)):
        wait(w_s.at[:, pl.ds(0, 2), :, cols_of(number)], w_side.at[number])
        wait(v_s.at[pl.ds(0, 2), :, cols_of(number)], v_side.at[number])
        along(number, v_on, w_stay_on, w_on)

    def panel_of(p, cols):
        block = w_s[p, :, :, cols]
        if w_s.shape[2] % 16:
            block = block.astype(F32)
        return block.reshape(panel, block.shape[-1]).astype(BF16)

    def products(at, stop):
        cols = pl.ds(at, stop - at)
        v = v_s[:, :, cols].reshape(rows, stop - at)
        first, second = panel_of(0, cols), panel_of(1, cols)
        part[:, :panel] += lax.dot_general(v, first, NT, preferred_element_type=F32)
        part[:, panel:2 * panel] += lax.dot_general(v, second, NT, preferred_element_type=F32)
        part[:, 2 * panel:] += lax.dot_general(first, second, NT, preferred_element_type=F32)

    for number in range(len(pieces)):
        wait(v_s.at[0, :, cols_of(number)], l_sem.at[number, 0])
        wait(w_s.at[:, 0, :, cols_of(number)], l_sem.at[number, 1])
        wait(v_s.at[pl.ds(0, 2), :, cols_of(number)], v_recv.at[number])
        wait(w_s.at[:, pl.ds(0, n_col - 2), :, cols_of(number)], w_recv.at[number])
        products(*sums_at[number])

    rs_send[...] = part[...].astype(BF16).reshape(rs_send.shape)
    for g, r, c in partners:
        remote(rs_send.at[g], rs_recv.at[me_g], r_send, r_recv, r, c).start()
    rs_recv[me_g] = rs_send[me_g]
    wait(rs_recv.at[pl.ds(0, group - 1)], r_recv)
    ag[me_g] = jnp.sum(rs_recv[...].astype(F32), axis=0).astype(BF16)
    for g, r, c in partners:
        remote(ag.at[me_g], ag.at[me_g], g_send, g_recv, r, c).start()
    keep_t.wait()
    wait(ag.at[pl.ds(0, group - 1)], g_recv)

    sums = ag[...].reshape(rows, 3 * panel)
    high = lax.Precision.HIGHEST
    s1 = lax.dot_general(
        sums[:, :panel].astype(F32), t_s[0], NT, precision=high, preferred_element_type=F32
    ).astype(BF16)
    p2 = sums[:, panel:2 * panel].astype(F32) - jnp.dot(
        s1, sums[:, 2 * panel:], preferred_element_type=F32
    )
    s2 = lax.dot_general(p2, t_s[1], NT, precision=high, preferred_element_type=F32).astype(BF16)
    s_s[0] = s1
    s_s[1] = s2

    def rows_of(r):
        return pl.ds(pl.multiple_of(r * own, own), own)

    for j, (at, stop) in enumerate(out_blocks):

        @pl.loop(at // n_block, stop // n_block)
        def _(i):
            cols = pl.ds(pl.multiple_of(i * n_block, n_block), n_block)
            v = v_s[:, :, cols].reshape(rows, n_block).astype(F32)
            v = v - jnp.dot(s_s[0], panel_of(0, cols), preferred_element_type=F32)
            v = v - jnp.dot(s_s[1], panel_of(1, cols), preferred_element_type=F32)
            v_s[:, :, cols] = v.astype(BF16).reshape(SPLIT, rows // SPLIT, n_block)

        cols = pl.ds(at, min(stop, site) - at)
        for g, r, c in partners:
            remote(
                v_s.at[lax.div(g, n_row), rows_of(r), cols], stage.at[me_g, :, cols],
                o_send, o_recv.at[j], r, c,
            ).start()

    for j, (at, stop) in enumerate(out_blocks):
        size = min(stop, site) - at
        cols = pl.ds(at, size)
        stage[me_g, :, cols] = v_s[me_a, rows_of(me_r), cols]
        wait(stage.at[pl.ds(0, group - 1), :, cols], o_recv.at[j])
        for r in range(n_row):
            for a in range(SPLIT):
                size = min(at + size, columns - a * site) - at
                begin = r * columns + a * site + at
                if size > 0:
                    o_ref[:, begin:begin + size] = stage[a * n_row + r, :, at:at + size]
                size = min(stop, site) - at
    wait(v_s.at[:, :, pl.ds(0, site)], v_send)
    wait(w_s.at[:, :, :, pl.ds(0, site)], w_send)
    wait(rs_recv.at[pl.ds(0, group - 1)], r_send)
    wait(ag.at[pl.ds(0, group - 1)], g_send)
    wait(stage.at[pl.ds(0, group - 1)], o_send)


def body(n_row, n_col, vectors, reflectors, panel_factor):
    own_rows, columns = vectors.shape
    part_rows, panel = reflectors.shape[1], panel_factor.shape[1]
    halves, group, rows = n_col // SPLIT, SPLIT * n_row, SPLIT * own_rows
    site = -(-columns // (SPLIT * LANES)) * LANES
    last = columns - (SPLIT - 1) * site
    main, rest = last // LANES * LANES, last % LANES
    n_block = 2 * LANES
    width = -(-site // n_block) * n_block
    step = -(-main // (4 * n_block)) * n_block
    cuts = list(range(0, main, step)) + [main]
    even = main // n_block * n_block
    pieces = tuple(zip(cuts[:-1], cuts[1:])) + ((main, site),)
    sums_at = tuple((s, min(e, even)) for s, e in pieces[:-1]) + ((even, width),)
    marks = [0, 2 * n_block]
    blocks = width // n_block
    marks += [n_block * (2 + (blocks - 2) * k // 6) for k in range(1, 7)]
    out_blocks = tuple(zip(marks[:-1], marks[1:]))
    edge = min(((SPLIT - 1) * site + main) // LANES, -(-columns // LANES) - 1)
    count = len(pieces)
    dma = pltpu.SemaphoreType.DMA
    plan = (site, main, rest, pieces, sums_at, out_blocks, n_block)
    whole = pl.pallas_call(
        functools.partial(kernel, n_row, n_col, columns, plan),
        grid=(1,),
        out_shape=jax.ShapeDtypeStruct((own_rows // n_row, n_row * columns), BF16),
        in_specs=[
            pl.BlockSpec(memory_space=pl.ANY),
            pl.BlockSpec(memory_space=pl.ANY),
            pl.BlockSpec((own_rows, LANES), lambda i: (0, edge)),
            pl.BlockSpec((2, part_rows, LANES), lambda i: (0, 0, edge)),
            pl.BlockSpec(memory_space=pltpu.HBM),
        ],
        out_specs=pl.BlockSpec(memory_space=pltpu.VMEM),
        scratch_shapes=[
            pltpu.VMEM((SPLIT, own_rows, width), BF16),
            pltpu.VMEM((2, n_col, part_rows, width), BF16),
            pltpu.VMEM((own_rows, site), BF16),
            pltpu.VMEM((2, part_rows, site), BF16),
            pltpu.VMEM((own_rows, site - main), BF16),
            pltpu.VMEM((2, part_rows, site - main), BF16),
            pltpu.VMEM(panel_factor.shape, F32),
            pltpu.VMEM((rows, 3 * panel), F32),
            pltpu.VMEM((group, rows // group, 3 * panel), BF16),
            pltpu.VMEM((group, rows // group, 3 * panel), BF16),
            pltpu.VMEM((group, rows // group, 3 * panel), BF16),
            pltpu.VMEM((2, rows, panel), BF16),
            pltpu.VMEM((group, own_rows // n_row, site), BF16),
            dma, dma, dma((count,)), dma((count,)), dma((count,)), dma((count,)), dma, dma, dma, dma,
            dma, dma((len(out_blocks),)), dma((count, 2)), dma,
        ],
        compiler_params=pltpu.CompilerParams(
            has_side_effects=True, collective_id=0, vmem_limit_bytes=48 * 1024 * 1024
        ),
        name="panels",
    )(
        vectors, reflectors, vectors, reflectors,
        pltpu.with_memory_space_constraint(panel_factor, pltpu.HBM),
    )
    return whole[None]


def solution(mesh):
    placed = (P("pcol", "prow"), P(None, "pcol", "prow"), P())
    return jax.shard_map(
        functools.partial(body, mesh.shape["prow"], mesh.shape["pcol"]),
        mesh=mesh, in_specs=placed, out_specs=P("pcol", "prow", None), check_vma=False,
    )
```

```python
import functools

import jax
import jax.numpy as jnp
from jax import lax
from jax.experimental import pallas as pl
from jax.experimental.pallas import tpu as pltpu
from jax.sharding import PartitionSpec as P

MESH = pl.DeviceIdType.MESH
LANES = 128
SPLIT = 4
F32, BF16 = jnp.float32, jnp.bfloat16
NT = (((1,), (1,)), ((), ()))


def flip(index, bit):
    return index + bit - 2 * bit * lax.rem(lax.div(index, bit), 2)


def flipped(index, mask):
    bit = 1
    while bit <= mask:
        if mask & bit:
            index = flip(index, bit)
        bit *= 2
    return index


def kernel(
    n_row, n_col, columns, plan,
    v_ref, w_ref, vt_ref, wt_ref, t_ref, o_ref,
    v_s, w_s, v_mid, w_mid, v_tail, w_tail, t_s, part, s_s, stage,
    m_send, m_recv, z_send, z_recv, m_all, rs_send, rs_recv, ag,
    v_sent, w_sent, v_came, w_came, v_side, w_side, l_sem, t_sem,
    m_sems, r_send, r_recv, g_send, g_recv, o_send, o_recv,
):
    site, main, rest, pieces, sums_at, out_blocks, n_block, early = plan
    me_r, me_c = lax.axis_index("prow"), lax.axis_index("pcol")
    me_a, me_b = lax.rem(me_c, SPLIT), lax.div(me_c, SPLIT)
    me_x, me_e = lax.rem(me_a, 2), lax.div(me_a, 2)
    halves, group, plane = n_col // SPLIT, SPLIT * n_row, 2 * n_row
    me_g, me_h = me_a * n_row + me_r, me_x * n_row + me_r
    inner = lax.rem(me_b + me_e, 2) == 1
    rows = SPLIT * v_s.shape[1]
    panel = w_s.shape[1] * w_s.shape[2]
    own = v_s.shape[1] // n_row
    side_c, side_a = flip(me_c, 1), flip(me_a, 1)
    far_a, side_far = flip(me_a, 2), flip(side_a, 2)
    far_c = me_b * SPLIT + far_a
    others = [lax.rem(me_b + k, halves) for k in range(1, halves)]
    numbers = range(len(pieces))

    def turns(mask):
        a, r = mask // n_row, mask % n_row
        first = 0 if a & 2 else 1 if a & 1 else 2 if r > 1 else 3
        size = -(bool(a & 1) * 2 + (r > 1)) if first == 0 else (r > 1)
        return first, size, mask

    def partner(mask):
        a, r = flipped(me_a, mask // n_row), flipped(me_r, mask % n_row)
        return a * n_row + r, r, me_b * SPLIT + a

    partners = [partner(mask) for mask in sorted(range(1, group), key=turns)]
    near_by = [partner(mask) for mask in sorted(range(1, plane), key=turns)]

    barrier = pltpu.get_barrier_semaphore()
    for _, r, c in partners:
        pl.semaphore_signal(barrier, device_id={"prow": r, "pcol": c}, device_id_type=MESH)
    for b in others:
        for a in (me_a, far_a):
            pl.semaphore_signal(
                barrier, device_id={"prow": me_r, "pcol": b * SPLIT + a}, device_id_type=MESH
            )

    def remote(src, dst, send, recv, r, c):
        return pltpu.make_async_remote_copy(
            src_ref=src, dst_ref=dst, send_sem=send, recv_sem=recv,
            device_id={"prow": r, "pcol": c}, device_id_type=MESH,
        )

    def wait(ref, sem):
        pltpu.make_async_copy(ref, ref, sem).wait()

    def cols_of(number):
        at, stop = pieces[number]
        return pl.ds(at, stop - at)

    def start(make, full, tail, q, number):
        at, stop = pieces[number]
        copy = make(full.at[..., pl.ds(pl.multiple_of(q * site + at, LANES), stop - at)])
        if at == main:
            pl.when(q == SPLIT - 1)(make(tail).start)
            pl.when(q != SPLIT - 1)(copy.start)
        else:
            copy.start()

    def v_slot(a):
        return lambda number: v_s.at[a, :, cols_of(number)]

    def w_slot(p, c):
        return lambda number: w_s.at[p, c, :, cols_of(number)]

    def v_half(number):
        return v_mid.at[:, cols_of(number)]

    def w_half(p):
        return lambda number: w_mid.at[p, :, cols_of(number)]

    def send_v(q, dst, come):
        def start_copy(number, c):
            start(
                lambda src: remote(src, dst(number), v_sent, come.at[number], me_r, c),
                v_ref, v_tail, q, number,
            )
        return start_copy

    def send_w(p, q, dst, come):
        def start_copy(number, c):
            start(
                lambda src: remote(src, dst(number), w_sent, come.at[p, number], me_r, c),
                w_ref.at[p], w_tail.at[p], q, number,
            )
        return start_copy

    def pass_v(src, dst):
        def start_copy(number, c):
            remote(src(number), dst(number), v_sent, v_came.at[number], me_r, c).start()
        return start_copy

    def pass_w(p, src, dst):
        def start_copy(number, c):
            remote(src(number), dst(number), w_sent, w_came.at[p, number], me_r, c).start()
        return start_copy

    keep_t = pltpu.make_async_copy(t_ref, t_s, t_sem)
    keep_t.start()
    v_tail[...] = jnp.zeros_like(v_tail)
    w_tail[...] = jnp.zeros_like(w_tail)
    if rest:
        v_tail[:, :rest] = vt_ref[:, :rest]
        w_tail[:, :, :rest] = wt_ref[:, :, :rest]
    width = v_s.shape[2]
    if width > site:
        v_s[:, :, site:] = jnp.zeros((SPLIT, v_s.shape[1], width - site), BF16)
        w_s[:, :, :, site:] = jnp.zeros((2, n_col, w_s.shape[2], width - site), BF16)
    part[...] = jnp.zeros_like(part)
    pl.semaphore_wait(barrier, len(partners) + 2 * len(others))

    v_own = v_slot(me_a)
    near_v = send_v(far_a, v_own, v_came)
    near_v_on = pass_v(v_half, v_slot(side_a))
    stay, across, stay_on, across_on = [], [], [], []
    for p in range(2):
        w_own, w_other = w_slot(p, me_c), w_slot(p, side_c)
        stay.append(send_w(p, me_a, w_own, w_came))
        across.append(send_w(p, far_a, w_own, w_came))
        stay_on.append(pass_w(p, w_other, w_other))
        across_on.append(pass_w(p, w_half(p), w_other))

    def far(number, here, there):
        for b in others:
            there(number, b * SPLIT + far_a)
            here(number, b * SPLIT + me_a)

    for number in numbers:
        far(number, stay[0], across[0])
        near_v(number, far_c)
        across[0](number, far_c)
        send_w(0, side_far, w_half(0), w_side)(number, side_c)
        send_v(side_far, v_half, v_side)(number, side_c)
        send_w(0, side_a, w_slot(0, me_c), w_side)(number, side_c)
        send_v(side_a, v_own, v_side)(number, side_c)
    for number in numbers:
        send_w(1, side_far, w_half(1), w_side)(number, side_c)
        send_w(1, side_a, w_slot(1, me_c), w_side)(number, side_c)
    for number in numbers:
        start(
            lambda src: pltpu.make_async_copy(src, v_own(number), l_sem.at[0]),
            v_ref, v_tail, me_a, number,
        )
        start(
            lambda src: pltpu.make_async_copy(src, w_s.at[:, me_c, :, cols_of(number)], l_sem.at[1]),
            w_ref, w_tail, me_a, number,
        )

    for number in numbers:
        wait(w_s.at[0, pl.ds(0, 2), :, cols_of(number)], w_side.at[0, number])
        wait(v_s.at[pl.ds(0, 2), :, cols_of(number)], v_side.at[number])
        far(number, stay_on[0], across_on[0])
        near_v_on(number, far_c)
        across_on[0](number, far_c)

    @pl.when(inner)
    def _():
        for number in numbers:
            for b in others:
                across[1](number, b * SPLIT + far_a)

    for number in numbers[:early]:

        @pl.when(jnp.logical_not(inner))
        def _():
            far(number, stay[1], across[1])

        across[1](number, far_c)
    for number in numbers:
        wait(w_s.at[1, pl.ds(0, 2), :, cols_of(number)], w_side.at[1, number])

        @pl.when(inner)
        def _():
            for b in others:
                across_on[1](number, b * SPLIT + far_a)

        if number < early:

            @pl.when(jnp.logical_not(inner))
            def _():
                far(number, stay_on[1], across_on[1])

            across_on[1](number, far_c)

    @pl.when(inner)
    def _():
        for number in numbers:
            for b in others:
                stay[1](number, b * SPLIT + me_a)
                stay_on[1](number, b * SPLIT + me_a)

    def panel_of(p, cols):
        block = w_s[p, :, :, cols]
        if w_s.shape[2] % 16:
            block = block.astype(F32)
        return block.reshape(panel, block.shape[-1]).astype(BF16)

    def products(p, at, stop):
        cols = pl.ds(at, stop - at)
        v = v_s[:, :, cols].reshape(rows, stop - at)
        part[...] += lax.dot_general(v, panel_of(p, cols), NT, preferred_element_type=F32)

    def factor_of(p, sums):
        s_s[...] = lax.dot_general(
            sums, t_s[p], NT, precision=lax.Precision.HIGHEST, preferred_element_type=F32
        ).astype(BF16)

    def update(p, at, stop):
        @pl.loop(at // n_block, stop // n_block)
        def _(i):
            cols = pl.ds(pl.multiple_of(i * n_block, n_block), n_block)
            v = v_s[:, :, cols].reshape(rows, n_block).astype(F32)
            v = v - jnp.dot(s_s[...], panel_of(p, cols), preferred_element_type=F32)
            v_s[:, :, cols] = v.astype(BF16).reshape(SPLIT, rows // SPLIT, n_block)

    wait(v_s.at[0, :, pl.ds(0, site)], l_sem.at[0])
    wait(w_s.at[:, 0, :, pl.ds(0, site)], l_sem.at[1])
    for number in numbers:
        wait(v_s.at[pl.ds(0, 2), :, cols_of(number)], v_came.at[number])
        wait(w_s.at[0, pl.ds(0, n_col - 2), :, cols_of(number)], w_came.at[0, number])
        products(0, *sums_at[number])

    m_send[...] = part[...].reshape(m_send.shape)
    part[...] = jnp.zeros_like(part)
    for g, r, c in near_by:
        h = lax.rem(g, plane)
        remote(m_send.at[h], m_recv.at[me_h], m_sems.at[0], m_sems.at[1], r, c).start()
    m_recv[me_h] = m_send[me_h]
    wait(m_recv.at[pl.ds(0, plane - 1)], m_sems.at[1])
    z_send[...] = jnp.sum(m_recv[...], axis=0)
    remote(z_send, z_recv, m_sems.at[2], m_sems.at[3], me_r, far_c).start()
    for number in numbers[early:]:

        @pl.when(jnp.logical_not(inner))
        def _():
            far(number, stay[1], across[1])

        across[1](number, far_c)

        @pl.when(jnp.logical_not(inner))
        def _():
            far(number, stay_on[1], across_on[1])

        across_on[1](number, far_c)
    wait(z_recv, m_sems.at[3])
    m_all[me_h] = z_send[...] + z_recv[...]
    for _, r, c in near_by:
        remote(m_all.at[me_h], m_all.at[me_h], m_sems.at[4], m_sems.at[5], r, c).start()
    keep_t.wait()
    wait(m_all.at[pl.ds(0, plane - 1)], m_sems.at[5])
    factor_of(0, m_all[...].reshape(rows, panel))
    update(0, 0, width)

    for number in numbers:
        wait(w_s.at[1, pl.ds(0, n_col - 2), :, cols_of(number)], w_came.at[1, number])
        products(1, *sums_at[number])

    rs_send[...] = part[...].astype(BF16).reshape(rs_send.shape)
    for g, r, c in partners:
        remote(rs_send.at[g], rs_recv.at[me_g], r_send, r_recv, r, c).start()
    rs_recv[me_g] = rs_send[me_g]
    wait(rs_recv.at[pl.ds(0, group - 1)], r_recv)
    ag[me_g] = jnp.sum(rs_recv[...].astype(F32), axis=0).astype(BF16)
    for g, r, c in partners:
        remote(ag.at[me_g], ag.at[me_g], g_send, g_recv, r, c).start()
    wait(ag.at[pl.ds(0, group - 1)], g_recv)
    factor_of(1, ag[...].reshape(rows, panel).astype(F32))

    def rows_of(r):
        return pl.ds(pl.multiple_of(r * own, own), own)

    for j, (at, stop) in enumerate(out_blocks):
        update(1, at, stop)
        cols = pl.ds(at, min(stop, site) - at)
        for g, r, c in partners:
            remote(
                v_s.at[lax.div(g, n_row), rows_of(r), cols], stage.at[me_g, :, cols],
                o_send, o_recv.at[j], r, c,
            ).start()

    for j, (at, stop) in enumerate(out_blocks):
        size = min(stop, site) - at
        cols = pl.ds(at, size)
        stage[me_g, :, cols] = v_s[me_a, rows_of(me_r), cols]
        wait(stage.at[pl.ds(0, group - 1), :, cols], o_recv.at[j])
        for r in range(n_row):
            for a in range(SPLIT):
                size = min(at + size, columns - a * site) - at
                begin = r * columns + a * site + at
                if size > 0:
                    o_ref[:, begin:begin + size] = stage[a * n_row + r, :, at:at + size]
                size = min(stop, site) - at
    wait(v_s.at[:, :, pl.ds(0, site)], v_sent)
    wait(w_s.at[:, :, :, pl.ds(0, site)], w_sent)
    wait(m_recv.at[pl.ds(0, plane - 1)], m_sems.at[0])
    wait(z_send, m_sems.at[2])
    wait(m_all.at[pl.ds(0, plane - 1)], m_sems.at[4])
    wait(rs_recv.at[pl.ds(0, group - 1)], r_send)
    wait(ag.at[pl.ds(0, group - 1)], g_send)
    wait(stage.at[pl.ds(0, group - 1)], o_send)


def body(n_row, n_col, vectors, reflectors, panel_factor):
    own_rows, columns = vectors.shape
    part_rows, panel = reflectors.shape[1], panel_factor.shape[1]
    group, plane, rows = SPLIT * n_row, 2 * n_row, SPLIT * own_rows
    site = -(-columns // (SPLIT * LANES)) * LANES
    last = columns - (SPLIT - 1) * site
    main, rest = last // LANES * LANES, last % LANES
    n_block = 2 * LANES
    width = -(-site // n_block) * n_block
    step = -(-main // (4 * n_block)) * n_block
    cuts = list(range(0, main, step)) + [main]
    even = main // n_block * n_block
    pieces = tuple(zip(cuts[:-1], cuts[1:])) + ((main, site),)
    sums_at = tuple((s, min(e, even)) for s, e in pieces[:-1]) + ((even, width),)
    marks = [0, 2 * n_block]
    blocks = width // n_block
    marks += [n_block * (2 + (blocks - 2) * k // 6) for k in range(1, 7)]
    out_blocks = tuple(zip(marks[:-1], marks[1:]))
    edge = min(((SPLIT - 1) * site + main) // LANES, -(-columns // LANES) - 1)
    count = len(pieces)
    dma = pltpu.SemaphoreType.DMA
    plan = (site, main, rest, pieces, sums_at, out_blocks, n_block, 2)
    whole = pl.pallas_call(
        functools.partial(kernel, n_row, n_col, columns, plan),
        grid=(1,),
        out_shape=jax.ShapeDtypeStruct((own_rows // n_row, n_row * columns), BF16),
        in_specs=[
            pl.BlockSpec(memory_space=pl.ANY),
            pl.BlockSpec(memory_space=pl.ANY),
            pl.BlockSpec((own_rows, LANES), lambda i: (0, edge)),
            pl.BlockSpec((2, part_rows, LANES), lambda i: (0, 0, edge)),
            pl.BlockSpec(memory_space=pltpu.HBM),
        ],
        out_specs=pl.BlockSpec(memory_space=pltpu.VMEM),
        scratch_shapes=[
            pltpu.VMEM((SPLIT, own_rows, width), BF16),
            pltpu.VMEM((2, n_col, part_rows, width), BF16),
            pltpu.VMEM((own_rows, site), BF16),
            pltpu.VMEM((2, part_rows, site), BF16),
            pltpu.VMEM((own_rows, site - main), BF16),
            pltpu.VMEM((2, part_rows, site - main), BF16),
            pltpu.VMEM(panel_factor.shape, F32),
            pltpu.VMEM((rows, panel), F32),
            pltpu.VMEM((rows, panel), BF16),
            pltpu.VMEM((group, own_rows // n_row, site), BF16),
            pltpu.VMEM((plane, rows // plane, panel), F32),
            pltpu.VMEM((plane, rows // plane, panel), F32),
            pltpu.VMEM((rows // plane, panel), F32),
            pltpu.VMEM((rows // plane, panel), F32),
            pltpu.VMEM((plane, rows // plane, panel), F32),
            pltpu.VMEM((group, rows // group, panel), BF16),
            pltpu.VMEM((group, rows // group, panel), BF16),
            pltpu.VMEM((group, rows // group, panel), BF16),
            dma, dma, dma((count,)), dma((2, count)), dma((count,)), dma((2, count)), dma((2,)), dma,
            dma((6,)), dma, dma, dma, dma, dma, dma((len(out_blocks),)),
        ],
        compiler_params=pltpu.CompilerParams(
            has_side_effects=True, collective_id=0, vmem_limit_bytes=48 * 1024 * 1024
        ),
        name="panels",
    )(
        vectors, reflectors, vectors, reflectors,
        pltpu.with_memory_space_constraint(panel_factor, pltpu.HBM),
    )
    return whole[None]


def solution(mesh):
    placed = (P("pcol", "prow"), P(None, "pcol", "prow"), P())
    return jax.shard_map(
        functools.partial(body, mesh.shape["prow"], mesh.shape["pcol"]),
        mesh=mesh, in_specs=placed, out_specs=P("pcol", "prow", None), check_vma=False,
    )
```

```python
import functools

import jax
import jax.numpy as jnp
from jax import lax
from jax.experimental import pallas as pl
from jax.experimental.pallas import tpu as pltpu
from jax.sharding import PartitionSpec as P

MESH = pl.DeviceIdType.MESH
LANES = 128
SPLIT = 4
F32, BF16 = jnp.float32, jnp.bfloat16
NT = (((1,), (1,)), ((), ()))


def flip(index, bit):
    return index + bit - 2 * bit * lax.rem(lax.div(index, bit), 2)


def flipped(index, mask):
    bit = 1
    while bit <= mask:
        if mask & bit:
            index = flip(index, bit)
        bit *= 2
    return index


def kernel(
    n_row, n_col, columns, plan,
    v_ref, w_ref, vt_ref, wt_ref, t_ref, o_ref,
    v_s, w_s, v_mid, w_mid, v_tail, w_tail, t_s, part, s_s, stage,
    m_send, m_recv, z_send, z_recv, m_all, rs_send, rs_recv, ag,
    v_sent, w_sent, v_came, w_came, v_side, w_side, l_sem, t_sem, lend_sent, lend_came,
    m_sems, r_send, r_recv, g_send, g_recv, o_send, o_recv, entered,
):
    site, main, rest, pieces, sums_at, out_blocks, n_block, early, lent = plan
    me_r, me_c = lax.axis_index("prow"), lax.axis_index("pcol")
    me_a, me_b = lax.rem(me_c, SPLIT), lax.div(me_c, SPLIT)
    me_x, me_e = lax.rem(me_a, 2), lax.div(me_a, 2)
    halves, group, plane = n_col // SPLIT, SPLIT * n_row, 2 * n_row
    me_g, me_h = me_a * n_row + me_r, me_x * n_row + me_r
    inner = lax.rem(me_b + me_e, 2) == 1
    rows = SPLIT * v_s.shape[1]
    panel = w_s.shape[1] * w_s.shape[2]
    own = v_s.shape[1] // n_row
    side_c, side_a = flip(me_c, 1), flip(me_a, 1)
    far_a, side_far = flip(me_a, 2), flip(side_a, 2)
    far_c = me_b * SPLIT + far_a
    others = [lax.rem(me_b + k, halves) for k in range(1, halves)]
    numbers = range(len(pieces))

    def turns(mask):
        a, r = mask // n_row, mask % n_row
        first = 0 if a & 2 else 1 if a & 1 else 2 if r > 1 else 3
        size = -(bool(a & 1) * 2 + (r > 1)) if first == 0 else (r > 1)
        return first, size, mask

    def partner(mask):
        a, r = flipped(me_a, mask // n_row), flipped(me_r, mask % n_row)
        return a * n_row + r, r, me_b * SPLIT + a

    masks = sorted(range(1, group), key=turns)
    partners = [partner(mask) for mask in masks]
    near_by = [partner(mask) for mask in masks if mask < plane]

    def earlier(mask):
        top = 1
        while 2 * top <= mask:
            top *= 2
        if top >= n_row:
            return lax.rem(lax.div(me_a, top // n_row), 2) == 1
        return lax.rem(lax.div(me_r, top), 2) == (0 if top == 1 else 1)

    met = [
        (earlier(mask), r, c, {n_row: 0, 2 * n_row: 1}.get(mask, 3))
        for mask, (_, r, c) in zip(masks, partners)
    ]
    met += [(b < me_b, me_r, b * SPLIT + a, 2) for b in others for a in (me_a, far_a)]
    ahead = [met[masks.index(n_row)][0], met[masks.index(2 * n_row)][0]]
    barrier = pltpu.get_barrier_semaphore()
    for early_one, r, c, _ in met:

        @pl.when(jnp.logical_not(early_one))
        def _():
            pl.semaphore_signal(barrier, device_id={"prow": r, "pcol": c}, device_id_type=MESH)

    def count_of(kind, early_ones):
        flags = [m[0] if early_ones else jnp.logical_not(m[0]) for m in met if kind in (m[3], None)]
        return sum(flag.astype(jnp.int32) for flag in flags)

    def wait_for(sem, count):
        pl.when(count > 0)(lambda: pl.semaphore_wait(sem, count))

    def remote(src, dst, send, recv, r, c):
        return pltpu.make_async_remote_copy(
            src_ref=src, dst_ref=dst, send_sem=send, recv_sem=recv,
            device_id={"prow": r, "pcol": c}, device_id_type=MESH,
        )

    def wait(ref, sem):
        pltpu.make_async_copy(ref, ref, sem).wait()

    def cols_of(number):
        at, stop = pieces[number]
        return pl.ds(at, stop - at)

    def start(make, full, tail, q, number):
        at, stop = pieces[number]
        copy = make(full.at[..., pl.ds(pl.multiple_of(q * site + at, LANES), stop - at)])
        if at == main:
            pl.when(q == SPLIT - 1)(make(tail).start)
            pl.when(q != SPLIT - 1)(copy.start)
        else:
            copy.start()

    def v_slot(a):
        return lambda number: v_s.at[a, :, cols_of(number)]

    def w_slot(p, c):
        return lambda number: w_s.at[p, c, :, cols_of(number)]

    def v_half(number):
        return v_mid.at[:, cols_of(number)]

    def w_half(p):
        return lambda number: w_mid.at[p, :, cols_of(number)]

    def sent_of(p, number):
        return 0 if p else 1 if number < lent else 2

    def send_v(q, dst, come):
        def start_copy(number, c):
            start(
                lambda src: remote(src, dst(number), v_sent, come.at[number], me_r, c),
                v_ref, v_tail, q, number,
            )
        return start_copy

    def send_w(p, q, dst, come):
        def start_copy(number, c):
            start(
                lambda src: remote(src, dst(number), w_sent.at[sent_of(p, number)], come.at[p, number], me_r, c),
                w_ref.at[p], w_tail.at[p], q, number,
            )
        return start_copy

    def pass_v(src, dst):
        def start_copy(number, c):
            remote(src(number), dst(number), v_sent, v_came.at[number], me_r, c).start()
        return start_copy

    def pass_w(p, src, dst):
        def start_copy(number, c):
            remote(
                src(number), dst(number), w_sent.at[sent_of(p, number)], w_came.at[p, number], me_r, c
            ).start()
        return start_copy

    keep_t = pltpu.make_async_copy(t_ref, t_s, t_sem)
    keep_t.start()
    v_tail[...] = jnp.zeros_like(v_tail)
    w_tail[...] = jnp.zeros_like(w_tail)
    if rest:
        v_tail[:, :rest] = vt_ref[:, :rest]
        w_tail[:, :, :rest] = wt_ref[:, :, :rest]
    width = v_s.shape[2]
    if width > site:
        v_s[:, :, site:] = jnp.zeros((SPLIT, v_s.shape[1], width - site), BF16)
        w_s[:, :, :, site:] = jnp.zeros((2, n_col, w_s.shape[2], width - site), BF16)
    part[...] = jnp.zeros_like(part)
    wait_for(barrier, count_of(None, True))
    for early_one, r, c, kind in met:

        @pl.when(early_one)
        def _():
            pl.semaphore_signal(
                entered.at[kind], device_id={"prow": r, "pcol": c}, device_id_type=MESH
            )

    v_own = v_slot(me_a)
    near_v = send_v(far_a, v_own, v_came)
    near_v_on = pass_v(v_half, v_slot(side_a))
    stay, across, stay_on, across_on = [], [], [], []
    for p in range(2):
        w_own, w_other = w_slot(p, me_c), w_slot(p, side_c)
        stay.append(send_w(p, me_a, w_own, w_came))
        across.append(send_w(p, far_a, w_own, w_came))
        stay_on.append(pass_w(p, w_other, w_other))
        across_on.append(pass_w(p, w_half(p), w_other))

    def far(number, here, there):
        for b in others:
            there(number, b * SPLIT + far_a)
            here(number, b * SPLIT + me_a)

    to_lender = send_w(0, far_a, w_slot(0, me_c), lend_came)

    def near(number):
        near_v(number, far_c)
        if number < lent:
            pl.when(inner)(functools.partial(across[0], number, far_c))
            pl.when(jnp.logical_not(inner))(functools.partial(to_lender, number, far_c))
        else:
            across[0](number, far_c)

    def over(number, c):
        if number < lent:

            @pl.when(inner)
            def _():
                start(
                    lambda src: remote(
                        src, w_slot(0, me_c)(number), lend_sent, w_came.at[0, number], me_r, c
                    ),
                    w_ref.at[0], w_tail.at[0], far_a, number,
                )
        else:
            across[0](number, c)

    for number in numbers:
        for b in others:

            @pl.when(b < me_b)
            def _():
                over(number, b * SPLIT + far_a)
                stay[0](number, b * SPLIT + me_a)

        pl.when(ahead[1])(functools.partial(near, number))
    wait_for(entered.at[0], count_of(0, False))
    for number in numbers:
        send_w(0, side_far, w_half(0), w_side)(number, side_c)
        send_v(side_far, v_half, v_side)(number, side_c)
        send_w(0, side_a, w_slot(0, me_c), w_side)(number, side_c)
        send_v(side_a, v_own, v_side)(number, side_c)
    for number in numbers:
        send_w(1, side_far, w_half(1), w_side)(number, side_c)
        send_w(1, side_a, w_slot(1, me_c), w_side)(number, side_c)
    wait_for(entered.at[1], count_of(1, False))
    pl.when(jnp.logical_not(ahead[1]))(functools.partial(near, 0))
    wait_for(entered.at[2], count_of(2, False))
    for number in numbers:
        for b in others:

            @pl.when(b > me_b)
            def _():
                over(number, b * SPLIT + far_a)
                stay[0](number, b * SPLIT + me_a)

        if number:
            pl.when(jnp.logical_not(ahead[1]))(functools.partial(near, number))
    @pl.when(inner)
    def _():
        for number in numbers:
            for b in others:
                across[1](number, b * SPLIT + far_a)

    for number in numbers:
        start(
            lambda src: pltpu.make_async_copy(src, v_own(number), l_sem.at[0]),
            v_ref, v_tail, me_a, number,
        )
        start(
            lambda src: pltpu.make_async_copy(src, w_s.at[:, me_c, :, cols_of(number)], l_sem.at[1]),
            w_ref, w_tail, me_a, number,
        )

    for number in numbers:
        wait(w_s.at[0, pl.ds(0, 2), :, cols_of(number)], w_side.at[0, number])
        wait(v_s.at[pl.ds(0, 2), :, cols_of(number)], v_side.at[number])
        far(number, stay_on[0], across_on[0])
        near_v_on(number, far_c)
        across_on[0](number, far_c)

    if lent:

        @pl.when(inner)
        def _():
            for number in numbers[:lent]:
                lend = w_slot(0, far_c)(number)
                wait(lend, lend_came.at[0, number])
                for b in others:
                    remote(
                        lend, lend, lend_sent, w_came.at[0, number], me_r, b * SPLIT + me_a
                    ).start()

    for number in numbers[:early]:

        @pl.when(jnp.logical_not(inner))
        def _():
            far(number, stay[1], across[1])

        across[1](number, far_c)
    for number in numbers:
        wait(w_s.at[1, pl.ds(0, 2), :, cols_of(number)], w_side.at[1, number])

        @pl.when(inner)
        def _():
            for b in others:
                across_on[1](number, b * SPLIT + far_a)

        if number < early:

            @pl.when(jnp.logical_not(inner))
            def _():
                far(number, stay_on[1], across_on[1])

            across_on[1](number, far_c)

    @pl.when(inner)
    def _():
        for number in numbers:
            for b in others:
                stay[1](number, b * SPLIT + me_a)
                stay_on[1](number, b * SPLIT + me_a)

    def panel_of(p, cols):
        block = w_s[p, :, :, cols]
        if w_s.shape[2] % 16:
            block = block.astype(F32)
        return block.reshape(panel, block.shape[-1]).astype(BF16)

    def products(p, at, stop):
        cols = pl.ds(at, stop - at)
        v = v_s[:, :, cols].reshape(rows, stop - at)
        part[...] += lax.dot_general(v, panel_of(p, cols), NT, preferred_element_type=F32)

    def factor_of(p, sums):
        return lax.dot_general(
            sums, t_s[p], NT, precision=lax.Precision.HIGHEST, preferred_element_type=F32
        ).astype(BF16)

    def update(p, at, stop):
        @pl.loop(at // n_block, stop // n_block)
        def _(i):
            cols = pl.ds(pl.multiple_of(i * n_block, n_block), n_block)
            v = v_s[:, :, cols].reshape(rows, n_block).astype(F32)
            v = v - jnp.dot(s_s[...], panel_of(p, cols), preferred_element_type=F32)
            v_s[:, :, cols] = v.astype(BF16).reshape(SPLIT, rows // SPLIT, n_block)

    wait(v_s.at[0, :, pl.ds(0, site)], l_sem.at[0])
    wait(w_s.at[:, 0, :, pl.ds(0, site)], l_sem.at[1])
    for number in numbers:
        wait(v_s.at[pl.ds(0, 2), :, cols_of(number)], v_came.at[number])
        if number < lent:
            for own_role, slots in ((inner, n_col - 3), (jnp.logical_not(inner), n_col - 2)):
                pl.when(own_role)(functools.partial(
                    wait, w_s.at[0, pl.ds(0, slots), :, cols_of(number)], w_came.at[0, number]
                ))
        else:
            wait(w_s.at[0, pl.ds(0, n_col - 2), :, cols_of(number)], w_came.at[0, number])
        products(0, *sums_at[number])

    m_send[...] = part[...].reshape(m_send.shape)
    wait_for(entered.at[3], count_of(3, False))
    part[...] = jnp.zeros_like(part)
    for g, r, c in near_by:
        h = lax.rem(g, plane)
        remote(m_send.at[h], m_recv.at[me_h], m_sems.at[0], m_sems.at[1], r, c).start()
    m_recv[me_h] = m_send[me_h]
    wait(m_recv.at[pl.ds(0, plane - 1)], m_sems.at[1])
    z_send[...] = jnp.sum(m_recv[...], axis=0)
    remote(z_send, z_recv, m_sems.at[2], m_sems.at[3], me_r, far_c).start()
    for number in numbers[early:]:

        @pl.when(jnp.logical_not(inner))
        def _():
            far(number, stay[1], across[1])

        across[1](number, far_c)

        @pl.when(jnp.logical_not(inner))
        def _():
            far(number, stay_on[1], across_on[1])

        across_on[1](number, far_c)
    wait(z_recv, m_sems.at[3])
    m_all[me_h] = z_send[...] + z_recv[...]
    for _, r, c in near_by:
        remote(m_all.at[me_h], m_all.at[me_h], m_sems.at[4], m_sems.at[5], r, c).start()
    keep_t.wait()
    wait(m_all.at[pl.ds(0, plane - 1)], m_sems.at[5])
    s_s[...] = factor_of(0, m_all[...].reshape(rows, panel))
    update(0, 0, width)

    for number in numbers:
        wait(w_s.at[1, pl.ds(0, n_col - 2), :, cols_of(number)], w_came.at[1, number])
        products(1, *sums_at[number])

    rs_send[...] = part[...].astype(BF16).reshape(rs_send.shape)
    for g, r, c in partners:
        remote(rs_send.at[g], rs_recv.at[me_g], r_send, r_recv, r, c).start()
    rs_recv[me_g] = rs_send[me_g]
    wait(rs_recv.at[pl.ds(0, group - 1)], r_recv)
    ag[me_g] = factor_of(1, jnp.sum(rs_recv[...].astype(F32), axis=0))
    for g, r, c in partners:
        remote(ag.at[me_g], ag.at[me_g], g_send, g_recv, r, c).start()
    wait(ag.at[pl.ds(0, group - 1)], g_recv)
    s_s[...] = ag[...].reshape(rows, panel)

    def rows_of(r):
        return pl.ds(pl.multiple_of(r * own, own), own)

    for j, (at, stop) in enumerate(out_blocks):
        update(1, at, stop)
        cols = pl.ds(at, min(stop, site) - at)
        for g, r, c in partners:
            remote(
                v_s.at[lax.div(g, n_row), rows_of(r), cols], stage.at[me_g, :, cols],
                o_send, o_recv.at[j], r, c,
            ).start()

    for j, (at, stop) in enumerate(out_blocks):
        size = min(stop, site) - at
        cols = pl.ds(at, size)
        stage[me_g, :, cols] = v_s[me_a, rows_of(me_r), cols]
        wait(stage.at[pl.ds(0, group - 1), :, cols], o_recv.at[j])
        for r in range(n_row):
            for a in range(SPLIT):
                size = min(at + size, columns - a * site) - at
                begin = r * columns + a * site + at
                if size > 0:
                    o_ref[:, begin:begin + size] = stage[a * n_row + r, :, at:at + size]
                size = min(stop, site) - at
    wait(v_s.at[:, :, pl.ds(0, site)], v_sent)
    cut = pieces[lent][0]
    wait(w_s.at[1, :, :, pl.ds(0, site)], w_sent.at[0])
    if lent:
        wait(w_s.at[0, pl.ds(0, n_col - len(others)), :, pl.ds(0, cut)], w_sent.at[1])

        @pl.when(inner)
        def _():
            wait(w_s.at[0, pl.ds(0, 2 * len(others)), :, pl.ds(0, cut)], lend_sent)

    wait(w_s.at[0, :, :, pl.ds(cut, site - cut)], w_sent.at[2])
    wait(m_recv.at[pl.ds(0, plane - 1)], m_sems.at[0])
    wait(z_send, m_sems.at[2])
    wait(m_all.at[pl.ds(0, plane - 1)], m_sems.at[4])
    wait(rs_recv.at[pl.ds(0, group - 1)], r_send)
    wait(ag.at[pl.ds(0, group - 1)], g_send)
    wait(stage.at[pl.ds(0, group - 1)], o_send)


def body(n_row, n_col, vectors, reflectors, panel_factor):
    own_rows, columns = vectors.shape
    part_rows, panel = reflectors.shape[1], panel_factor.shape[1]
    group, plane, rows = SPLIT * n_row, 2 * n_row, SPLIT * own_rows
    site = -(-columns // (SPLIT * LANES)) * LANES
    last = columns - (SPLIT - 1) * site
    main, rest = last // LANES * LANES, last % LANES
    n_block = 2 * LANES
    width = -(-site // n_block) * n_block
    step = -(-main // (4 * n_block)) * n_block
    cuts = list(range(0, main, step)) + [main]
    even = main // n_block * n_block
    pieces = tuple(zip(cuts[:-1], cuts[1:])) + ((main, site),)
    sums_at = tuple((s, min(e, even)) for s, e in pieces[:-1]) + ((even, width),)
    marks = [0, 2 * n_block]
    blocks = width // n_block
    marks += [n_block * (2 + (blocks - 2) * k // 6) for k in range(1, 7)]
    out_blocks = tuple(zip(marks[:-1], marks[1:]))
    edge = min(((SPLIT - 1) * site + main) // LANES, -(-columns // LANES) - 1)
    count = len(pieces)
    dma = pltpu.SemaphoreType.DMA
    plan = (site, main, rest, pieces, sums_at, out_blocks, n_block, 2, 2)
    whole = pl.pallas_call(
        functools.partial(kernel, n_row, n_col, columns, plan),
        grid=(1,),
        out_shape=jax.ShapeDtypeStruct((own_rows // n_row, n_row * columns), BF16),
        in_specs=[
            pl.BlockSpec(memory_space=pl.ANY),
            pl.BlockSpec(memory_space=pl.ANY),
            pl.BlockSpec((own_rows, LANES), lambda i: (0, edge)),
            pl.BlockSpec((2, part_rows, LANES), lambda i: (0, 0, edge)),
            pl.BlockSpec(memory_space=pltpu.HBM),
        ],
        out_specs=pl.BlockSpec(memory_space=pltpu.VMEM),
        scratch_shapes=[
            pltpu.VMEM((SPLIT, own_rows, width), BF16),
            pltpu.VMEM((2, n_col, part_rows, width), BF16),
            pltpu.VMEM((own_rows, site), BF16),
            pltpu.VMEM((2, part_rows, site), BF16),
            pltpu.VMEM((own_rows, site - main), BF16),
            pltpu.VMEM((2, part_rows, site - main), BF16),
            pltpu.VMEM(panel_factor.shape, F32),
            pltpu.VMEM((rows, panel), F32),
            pltpu.VMEM((rows, panel), BF16),
            pltpu.VMEM((group, own_rows // n_row, site), BF16),
            pltpu.VMEM((plane, rows // plane, panel), F32),
            pltpu.VMEM((plane, rows // plane, panel), F32),
            pltpu.VMEM((rows // plane, panel), F32),
            pltpu.VMEM((rows // plane, panel), F32),
            pltpu.VMEM((plane, rows // plane, panel), F32),
            pltpu.VMEM((group, rows // group, panel), BF16),
            pltpu.VMEM((group, rows // group, panel), BF16),
            pltpu.VMEM((group, rows // group, panel), BF16),
            dma, dma((3,)), dma((count,)), dma((2, count)), dma((count,)), dma((2, count)), dma((2,)), dma,
            dma, dma((1, count)),
            dma((6,)), dma, dma, dma, dma, dma, dma((len(out_blocks),)),
            pltpu.SemaphoreType.REGULAR((4,)),
        ],
        compiler_params=pltpu.CompilerParams(
            has_side_effects=True, collective_id=0, vmem_limit_bytes=48 * 1024 * 1024
        ),
        name="panels",
    )(
        vectors, reflectors, vectors, reflectors,
        pltpu.with_memory_space_constraint(panel_factor, pltpu.HBM),
    )
    return whole[None]


def solution(mesh):
    placed = (P("pcol", "prow"), P(None, "pcol", "prow"), P())
    return jax.shard_map(
        functools.partial(body, mesh.shape["prow"], mesh.shape["pcol"]),
        mesh=mesh, in_specs=placed, out_specs=P("pcol", "prow", None), check_vma=False,
    )
```

```python
import functools

import jax
import jax.numpy as jnp
from jax import lax
from jax.experimental import pallas as pl
from jax.experimental.pallas import tpu as pltpu
from jax.sharding import PartitionSpec as P

MESH = pl.DeviceIdType.MESH
LANES = 128
SPLIT = 4
F32, BF16 = jnp.float32, jnp.bfloat16
NT = (((1,), (1,)), ((), ()))


def flip(index, bit):
    return index + bit - 2 * bit * lax.rem(lax.div(index, bit), 2)


def flipped(index, mask):
    bit = 1
    while bit <= mask:
        if mask & bit:
            index = flip(index, bit)
        bit *= 2
    return index


def kernel(
    n_row, n_col, columns, plan,
    v_ref, w_ref, vt_ref, wt_ref, t_ref, o_ref,
    v_s, w_s, v_mid, w_mid, v_tail, w_tail, t_s, part, s_s, stage,
    m_send, m_recv, z_send, z_recv, m_all, rs_send, rs_recv, ag,
    v_sent, w_sent, v_came, w_came, v_side, w_side, l_sem, t_sem, lend_sent, lend_came,
    m_sems, r_send, r_recv, g_send, g_recv, o_send, o_recv, entered, told,
):
    site, main, rest, pieces, sums_at, out_blocks, n_block, early, lent = plan
    me_r, me_c = lax.axis_index("prow"), lax.axis_index("pcol")
    me_a, me_b = lax.rem(me_c, SPLIT), lax.div(me_c, SPLIT)
    me_x, me_e = lax.rem(me_a, 2), lax.div(me_a, 2)
    halves, group, plane = n_col // SPLIT, SPLIT * n_row, 2 * n_row
    me_g, me_h = me_a * n_row + me_r, me_x * n_row + me_r
    inner = lax.rem(me_b + me_e, 2) == 1
    rows = SPLIT * v_s.shape[1]
    panel = w_s.shape[1] * w_s.shape[2]
    own = v_s.shape[1] // n_row
    side_c, side_a = flip(me_c, 1), flip(me_a, 1)
    far_a, side_far = flip(me_a, 2), flip(side_a, 2)
    far_c = me_b * SPLIT + far_a
    others = [lax.rem(me_b + k, halves) for k in range(1, halves)]
    numbers = range(len(pieces))

    def turns(mask):
        a, r = mask // n_row, mask % n_row
        first = 0 if a & 2 else 1 if a & 1 else 2 if r > 1 else 3
        size = -(bool(a & 1) * 2 + (r > 1)) if first == 0 else (r > 1)
        return first, size, mask

    def partner(mask):
        a, r = flipped(me_a, mask // n_row), flipped(me_r, mask % n_row)
        return a * n_row + r, r, me_b * SPLIT + a

    masks = sorted(range(1, group), key=turns)
    partners = [partner(mask) for mask in masks]
    near_by = [partner(mask) for mask in masks if mask < plane]

    def earlier(mask):
        top = 1
        while 2 * top <= mask:
            top *= 2
        if top >= n_row:
            return lax.rem(lax.div(me_a, top // n_row), 2) == 1
        return lax.rem(lax.div(me_r, top), 2) == (0 if top == 1 else 1)

    steps = [1 << bit for bit in range(group.bit_length() - 1)]
    met = [
        (earlier(mask), *partner(mask)[1:], {n_row: 0, 2 * n_row: 1}.get(mask, 3))
        for mask in steps
    ]
    met += [(b < me_b, me_r, b * SPLIT + a, 2) for b in others for a in (me_a, far_a)]
    ahead = [earlier(n_row), earlier(2 * n_row)]
    barrier = pltpu.get_barrier_semaphore()
    for early_one, r, c, _ in met:

        @pl.when(jnp.logical_not(early_one))
        def _():
            pl.semaphore_signal(barrier, device_id={"prow": r, "pcol": c}, device_id_type=MESH)

    def count_of(kind, early_ones):
        flags = [m[0] if early_ones else jnp.logical_not(m[0]) for m in met if kind in (m[3], None)]
        return sum(flag.astype(jnp.int32) for flag in flags)

    def wait_for(sem, count):
        pl.when(count > 0)(lambda: pl.semaphore_wait(sem, count))

    def remote(src, dst, send, recv, r, c):
        return pltpu.make_async_remote_copy(
            src_ref=src, dst_ref=dst, send_sem=send, recv_sem=recv,
            device_id={"prow": r, "pcol": c}, device_id_type=MESH,
        )

    def wait(ref, sem):
        pltpu.make_async_copy(ref, ref, sem).wait()

    def cols_of(number):
        at, stop = pieces[number]
        return pl.ds(at, stop - at)

    def start(make, full, tail, q, number):
        at, stop = pieces[number]
        copy = make(full.at[..., pl.ds(pl.multiple_of(q * site + at, LANES), stop - at)])
        if at == main:
            pl.when(q == SPLIT - 1)(make(tail).start)
            pl.when(q != SPLIT - 1)(copy.start)
        else:
            copy.start()

    def v_slot(a):
        return lambda number: v_s.at[a, :, cols_of(number)]

    def w_slot(p, c):
        return lambda number: w_s.at[p, c, :, cols_of(number)]

    def v_half(number):
        return v_mid.at[:, cols_of(number)]

    def w_half(p):
        return lambda number: w_mid.at[p, :, cols_of(number)]

    def sent_of(p, number):
        return 0 if p else 1 if number < lent else 2

    def send_v(q, dst, come):
        def start_copy(number, c):
            start(
                lambda src: remote(src, dst(number), v_sent, come.at[number], me_r, c),
                v_ref, v_tail, q, number,
            )
        return start_copy

    def send_w(p, q, dst, come):
        def start_copy(number, c):
            start(
                lambda src: remote(src, dst(number), w_sent.at[sent_of(p, number)], come.at[p, number], me_r, c),
                w_ref.at[p], w_tail.at[p], q, number,
            )
        return start_copy

    def pass_v(src, dst):
        def start_copy(number, c):
            remote(src(number), dst(number), v_sent, v_came.at[number], me_r, c).start()
        return start_copy

    def pass_w(p, src, dst):
        def start_copy(number, c):
            remote(
                src(number), dst(number), w_sent.at[sent_of(p, number)], w_came.at[p, number], me_r, c
            ).start()
        return start_copy

    keep_t = pltpu.make_async_copy(t_ref, t_s, t_sem)
    keep_t.start()
    v_tail[...] = jnp.zeros_like(v_tail)
    w_tail[...] = jnp.zeros_like(w_tail)
    if rest:
        v_tail[:, :rest] = vt_ref[:, :rest]
        w_tail[:, :, :rest] = wt_ref[:, :, :rest]
    width = v_s.shape[2]
    if width > site:
        v_s[:, :, site:] = jnp.zeros((SPLIT, v_s.shape[1], width - site), BF16)
        w_s[:, :, :, site:] = jnp.zeros((2, n_col, w_s.shape[2], width - site), BF16)
    part[...] = jnp.zeros_like(part)
    wait_for(barrier, count_of(None, True))
    for early_one, r, c, kind in met:

        @pl.when(early_one)
        def _():
            pl.semaphore_signal(
                entered.at[kind], device_id={"prow": r, "pcol": c}, device_id_type=MESH
            )

    v_own = v_slot(me_a)
    near_v = send_v(far_a, v_own, v_came)
    near_v_on = pass_v(v_half, v_slot(side_a))
    stay, across, stay_on, across_on = [], [], [], []
    for p in range(2):
        w_own, w_other = w_slot(p, me_c), w_slot(p, side_c)
        stay.append(send_w(p, me_a, w_own, w_came))
        across.append(send_w(p, far_a, w_own, w_came))
        stay_on.append(pass_w(p, w_other, w_other))
        across_on.append(pass_w(p, w_half(p), w_other))

    def far(number, here, there):
        for b in others:
            there(number, b * SPLIT + far_a)
            here(number, b * SPLIT + me_a)

    to_lender = send_w(0, far_a, w_slot(0, me_c), lend_came)

    def near(number):
        near_v(number, far_c)
        if number < lent:
            pl.when(inner)(functools.partial(across[0], number, far_c))
            pl.when(jnp.logical_not(inner))(functools.partial(to_lender, number, far_c))
        else:
            across[0](number, far_c)

    def over(number, c):
        if number < lent:

            @pl.when(inner)
            def _():
                start(
                    lambda src: remote(
                        src, w_slot(0, me_c)(number), lend_sent, w_came.at[0, number], me_r, c
                    ),
                    w_ref.at[0], w_tail.at[0], far_a, number,
                )
        else:
            across[0](number, c)

    for number in numbers:
        for b in others:

            @pl.when(b < me_b)
            def _():
                over(number, b * SPLIT + far_a)
                stay[0](number, b * SPLIT + me_a)

        pl.when(ahead[1])(functools.partial(near, number))
    wait_for(entered.at[0], count_of(0, False))
    for number in numbers:
        send_w(0, side_far, w_half(0), w_side)(number, side_c)
        send_v(side_far, v_half, v_side)(number, side_c)
        send_w(0, side_a, w_slot(0, me_c), w_side)(number, side_c)
        send_v(side_a, v_own, v_side)(number, side_c)
    for number in numbers:
        send_w(1, side_far, w_half(1), w_side)(number, side_c)
        send_w(1, side_a, w_slot(1, me_c), w_side)(number, side_c)
    wait_for(entered.at[1], count_of(1, False))
    pl.when(jnp.logical_not(ahead[1]))(functools.partial(near, 0))
    wait_for(entered.at[2], count_of(2, False))
    for number in numbers:
        for b in others:

            @pl.when(b > me_b)
            def _():
                over(number, b * SPLIT + far_a)
                stay[0](number, b * SPLIT + me_a)

        if number:
            pl.when(jnp.logical_not(ahead[1]))(functools.partial(near, number))
    @pl.when(inner)
    def _():
        for number in numbers:
            for b in others:
                across[1](number, b * SPLIT + far_a)

    for number in numbers:
        start(
            lambda src: pltpu.make_async_copy(src, v_own(number), l_sem.at[0]),
            v_ref, v_tail, me_a, number,
        )
        start(
            lambda src: pltpu.make_async_copy(src, w_s.at[:, me_c, :, cols_of(number)], l_sem.at[1]),
            w_ref, w_tail, me_a, number,
        )

    for number in numbers:
        wait(w_s.at[0, pl.ds(0, 2), :, cols_of(number)], w_side.at[0, number])
        wait(v_s.at[pl.ds(0, 2), :, cols_of(number)], v_side.at[number])
        far(number, stay_on[0], across_on[0])
        near_v_on(number, far_c)
        across_on[0](number, far_c)

    if lent:

        @pl.when(inner)
        def _():
            for number in numbers[:lent]:
                lend = w_slot(0, far_c)(number)
                wait(lend, lend_came.at[0, number])
                for b in others:
                    remote(
                        lend, lend, lend_sent, w_came.at[0, number], me_r, b * SPLIT + me_a
                    ).start()

    for number in numbers[:early]:

        @pl.when(jnp.logical_not(inner))
        def _():
            far(number, stay[1], across[1])

        across[1](number, far_c)
    for number in numbers:
        wait(w_s.at[1, pl.ds(0, 2), :, cols_of(number)], w_side.at[1, number])

        @pl.when(inner)
        def _():
            for b in others:
                across_on[1](number, b * SPLIT + far_a)

        if number < early:

            @pl.when(jnp.logical_not(inner))
            def _():
                far(number, stay_on[1], across_on[1])

            across_on[1](number, far_c)

    @pl.when(inner)
    def _():
        for number in numbers:
            for b in others:
                stay[1](number, b * SPLIT + me_a)
                stay_on[1](number, b * SPLIT + me_a)

    wait_for(entered.at[3], count_of(3, False))
    for k, mask in enumerate(steps):
        _, r, c = partner(mask)
        pl.semaphore_signal(told.at[k], device_id={"prow": r, "pcol": c}, device_id_type=MESH)
        pl.semaphore_wait(told.at[k], 1)

    def panel_of(p, cols):
        block = w_s[p, :, :, cols]
        if w_s.shape[2] % 16:
            block = block.astype(F32)
        return block.reshape(panel, block.shape[-1]).astype(BF16)

    def products(p, at, stop):
        cols = pl.ds(at, stop - at)
        v = v_s[:, :, cols].reshape(rows, stop - at)
        part[...] += lax.dot_general(v, panel_of(p, cols), NT, preferred_element_type=F32)

    def factor_of(p, sums):
        return lax.dot_general(
            sums, t_s[p], NT, precision=lax.Precision.HIGHEST, preferred_element_type=F32
        ).astype(BF16)

    def update(p, at, stop):
        @pl.loop(at // n_block, stop // n_block)
        def _(i):
            cols = pl.ds(pl.multiple_of(i * n_block, n_block), n_block)
            v = v_s[:, :, cols].reshape(rows, n_block).astype(F32)
            v = v - jnp.dot(s_s[...], panel_of(p, cols), preferred_element_type=F32)
            v_s[:, :, cols] = v.astype(BF16).reshape(SPLIT, rows // SPLIT, n_block)

    wait(v_s.at[0, :, pl.ds(0, site)], l_sem.at[0])
    wait(w_s.at[:, 0, :, pl.ds(0, site)], l_sem.at[1])
    for number in numbers:
        wait(v_s.at[pl.ds(0, 2), :, cols_of(number)], v_came.at[number])
        if number < lent:
            for own_role, slots in ((inner, n_col - 3), (jnp.logical_not(inner), n_col - 2)):
                pl.when(own_role)(functools.partial(
                    wait, w_s.at[0, pl.ds(0, slots), :, cols_of(number)], w_came.at[0, number]
                ))
        else:
            wait(w_s.at[0, pl.ds(0, n_col - 2), :, cols_of(number)], w_came.at[0, number])
        products(0, *sums_at[number])

    m_send[...] = part[...].reshape(m_send.shape)
    part[...] = jnp.zeros_like(part)
    for g, r, c in near_by:
        h = lax.rem(g, plane)
        remote(m_send.at[h], m_recv.at[me_h], m_sems.at[0], m_sems.at[1], r, c).start()
    m_recv[me_h] = m_send[me_h]
    wait(m_recv.at[pl.ds(0, plane - 1)], m_sems.at[1])
    z_send[...] = jnp.sum(m_recv[...], axis=0)
    remote(z_send, z_recv, m_sems.at[2], m_sems.at[3], me_r, far_c).start()
    for number in numbers[early:]:

        @pl.when(jnp.logical_not(inner))
        def _():
            far(number, stay[1], across[1])

        across[1](number, far_c)

        @pl.when(jnp.logical_not(inner))
        def _():
            far(number, stay_on[1], across_on[1])

        across_on[1](number, far_c)
    wait(z_recv, m_sems.at[3])
    m_all[me_h] = z_send[...] + z_recv[...]
    for _, r, c in near_by:
        remote(m_all.at[me_h], m_all.at[me_h], m_sems.at[4], m_sems.at[5], r, c).start()
    keep_t.wait()
    wait(m_all.at[pl.ds(0, plane - 1)], m_sems.at[5])
    s_s[...] = factor_of(0, m_all[...].reshape(rows, panel))
    update(0, 0, width)

    for number in numbers:
        wait(w_s.at[1, pl.ds(0, n_col - 2), :, cols_of(number)], w_came.at[1, number])
        products(1, *sums_at[number])

    rs_send[...] = part[...].astype(BF16).reshape(rs_send.shape)
    for g, r, c in partners:
        remote(rs_send.at[g], rs_recv.at[me_g], r_send, r_recv, r, c).start()
    rs_recv[me_g] = rs_send[me_g]
    wait(rs_recv.at[pl.ds(0, group - 1)], r_recv)
    ag[me_g] = factor_of(1, jnp.sum(rs_recv[...].astype(F32), axis=0))
    for g, r, c in partners:
        remote(ag.at[me_g], ag.at[me_g], g_send, g_recv, r, c).start()
    wait(ag.at[pl.ds(0, group - 1)], g_recv)
    s_s[...] = ag[...].reshape(rows, panel)

    def rows_of(r):
        return pl.ds(pl.multiple_of(r * own, own), own)

    for j, (at, stop) in enumerate(out_blocks):
        update(1, at, stop)
        cols = pl.ds(at, min(stop, site) - at)
        for g, r, c in partners:
            remote(
                v_s.at[lax.div(g, n_row), rows_of(r), cols], stage.at[me_g, :, cols],
                o_send, o_recv.at[j], r, c,
            ).start()

    for j, (at, stop) in enumerate(out_blocks):
        size = min(stop, site) - at
        cols = pl.ds(at, size)
        stage[me_g, :, cols] = v_s[me_a, rows_of(me_r), cols]
        wait(stage.at[pl.ds(0, group - 1), :, cols], o_recv.at[j])
        for r in range(n_row):
            for a in range(SPLIT):
                size = min(at + size, columns - a * site) - at
                begin = r * columns + a * site + at
                if size > 0:
                    o_ref[:, begin:begin + size] = stage[a * n_row + r, :, at:at + size]
                size = min(stop, site) - at
    wait(v_s.at[:, :, pl.ds(0, site)], v_sent)
    cut = pieces[lent][0]
    wait(w_s.at[1, :, :, pl.ds(0, site)], w_sent.at[0])
    if lent:
        wait(w_s.at[0, pl.ds(0, n_col - len(others)), :, pl.ds(0, cut)], w_sent.at[1])

        @pl.when(inner)
        def _():
            wait(w_s.at[0, pl.ds(0, 2 * len(others)), :, pl.ds(0, cut)], lend_sent)

    wait(w_s.at[0, :, :, pl.ds(cut, site - cut)], w_sent.at[2])
    wait(m_recv.at[pl.ds(0, plane - 1)], m_sems.at[0])
    wait(z_send, m_sems.at[2])
    wait(m_all.at[pl.ds(0, plane - 1)], m_sems.at[4])
    wait(rs_recv.at[pl.ds(0, group - 1)], r_send)
    wait(ag.at[pl.ds(0, group - 1)], g_send)
    wait(stage.at[pl.ds(0, group - 1)], o_send)


def body(n_row, n_col, vectors, reflectors, panel_factor):
    own_rows, columns = vectors.shape
    part_rows, panel = reflectors.shape[1], panel_factor.shape[1]
    group, plane, rows = SPLIT * n_row, 2 * n_row, SPLIT * own_rows
    site = -(-columns // (SPLIT * LANES)) * LANES
    last = columns - (SPLIT - 1) * site
    main, rest = last // LANES * LANES, last % LANES
    n_block = 2 * LANES
    width = -(-site // n_block) * n_block
    step = -(-main // (4 * n_block)) * n_block
    cuts = list(range(0, main, step)) + [main]
    even = main // n_block * n_block
    pieces = tuple(zip(cuts[:-1], cuts[1:])) + ((main, site),)
    sums_at = tuple((s, min(e, even)) for s, e in pieces[:-1]) + ((even, width),)
    marks = [0, 2 * n_block]
    blocks = width // n_block
    marks += [n_block * (2 + (blocks - 2) * k // 6) for k in range(1, 7)]
    out_blocks = tuple(zip(marks[:-1], marks[1:]))
    edge = min(((SPLIT - 1) * site + main) // LANES, -(-columns // LANES) - 1)
    count = len(pieces)
    dma = pltpu.SemaphoreType.DMA
    plan = (site, main, rest, pieces, sums_at, out_blocks, n_block, 2, 2)
    whole = pl.pallas_call(
        functools.partial(kernel, n_row, n_col, columns, plan),
        grid=(1,),
        out_shape=jax.ShapeDtypeStruct((own_rows // n_row, n_row * columns), BF16),
        in_specs=[
            pl.BlockSpec(memory_space=pl.ANY),
            pl.BlockSpec(memory_space=pl.ANY),
            pl.BlockSpec((own_rows, LANES), lambda i: (0, edge)),
            pl.BlockSpec((2, part_rows, LANES), lambda i: (0, 0, edge)),
            pl.BlockSpec(memory_space=pltpu.HBM),
        ],
        out_specs=pl.BlockSpec(memory_space=pltpu.VMEM),
        scratch_shapes=[
            pltpu.VMEM((SPLIT, own_rows, width), BF16),
            pltpu.VMEM((2, n_col, part_rows, width), BF16),
            pltpu.VMEM((own_rows, site), BF16),
            pltpu.VMEM((2, part_rows, site), BF16),
            pltpu.VMEM((own_rows, site - main), BF16),
            pltpu.VMEM((2, part_rows, site - main), BF16),
            pltpu.VMEM(panel_factor.shape, F32),
            pltpu.VMEM((rows, panel), F32),
            pltpu.VMEM((rows, panel), BF16),
            pltpu.VMEM((group, own_rows // n_row, site), BF16),
            pltpu.VMEM((plane, rows // plane, panel), F32),
            pltpu.VMEM((plane, rows // plane, panel), F32),
            pltpu.VMEM((rows // plane, panel), F32),
            pltpu.VMEM((rows // plane, panel), F32),
            pltpu.VMEM((plane, rows // plane, panel), F32),
            pltpu.VMEM((group, rows // group, panel), BF16),
            pltpu.VMEM((group, rows // group, panel), BF16),
            pltpu.VMEM((group, rows // group, panel), BF16),
            dma, dma((3,)), dma((count,)), dma((2, count)), dma((count,)), dma((2, count)), dma((2,)), dma,
            dma, dma((1, count)),
            dma((6,)), dma, dma, dma, dma, dma, dma((len(out_blocks),)),
            pltpu.SemaphoreType.REGULAR((4,)),
            pltpu.SemaphoreType.REGULAR((group.bit_length() - 1,)),
        ],
        compiler_params=pltpu.CompilerParams(
            has_side_effects=True, collective_id=0, vmem_limit_bytes=48 * 1024 * 1024
        ),
        name="panels",
    )(
        vectors, reflectors, vectors, reflectors,
        pltpu.with_memory_space_constraint(panel_factor, pltpu.HBM),
    )
    return whole[None]


def solution(mesh):
    placed = (P("pcol", "prow"), P(None, "pcol", "prow"), P())
    return jax.shard_map(
        functools.partial(body, mesh.shape["prow"], mesh.shape["pcol"]),
        mesh=mesh, in_specs=placed, out_specs=P("pcol", "prow", None), check_vma=False,
    )
```

```python
import functools

import jax
import jax.numpy as jnp
from jax import lax
from jax.experimental import pallas as pl
from jax.experimental.pallas import tpu as pltpu
from jax.sharding import PartitionSpec as P

MESH = pl.DeviceIdType.MESH
LANES = 128
SPLIT = 4
F32, BF16 = jnp.float32, jnp.bfloat16
NT = (((1,), (1,)), ((), ()))


def flip(index, bit):
    return index + bit - 2 * bit * lax.rem(lax.div(index, bit), 2)


def flipped(index, mask):
    bit = 1
    while bit <= mask:
        if mask & bit:
            index = flip(index, bit)
        bit *= 2
    return index


def kernel(
    n_row, n_col, columns, plan,
    v_ref, w_ref, t_ref, o_ref,
    v_s, w_s, v_mid, w_mid, v_tail, w_tail, v_all, w_all, t_s, part, s_s, stage,
    m_send, m_recv, z_send, z_recv, m_all, rs_send, rs_recv, ag,
    v_sent, w_sent, v_came, w_came, v_side, w_side, l_sem, t_sem, lend_sent, lend_came,
    m_sems, r_send, r_recv, g_send, g_recv, o_send, o_recv, entered, told,
):
    site, main, rest, pieces, sums_at, out_blocks, n_block, early, lent = plan
    me_r, me_c = lax.axis_index("prow"), lax.axis_index("pcol")
    me_a, me_b = lax.rem(me_c, SPLIT), lax.div(me_c, SPLIT)
    me_x, me_e = lax.rem(me_a, 2), lax.div(me_a, 2)
    halves, group, plane = n_col // SPLIT, SPLIT * n_row, 2 * n_row
    me_g, me_h = me_a * n_row + me_r, me_x * n_row + me_r
    inner = lax.rem(me_b + me_e, 2) == 1
    rows = SPLIT * v_s.shape[1]
    panel = w_s.shape[1] * w_s.shape[2]
    own = v_s.shape[1] // n_row
    side_c, side_a = flip(me_c, 1), flip(me_a, 1)
    far_a, side_far = flip(me_a, 2), flip(side_a, 2)
    far_c = me_b * SPLIT + far_a
    others = [lax.rem(me_b + k, halves) for k in range(1, halves)]
    numbers = range(len(pieces))

    def turns(mask):
        a, r = mask // n_row, mask % n_row
        first = 0 if a & 2 else 1 if a & 1 else 2 if r > 1 else 3
        size = -(bool(a & 1) * 2 + (r > 1)) if first == 0 else (r > 1)
        return first, size, mask

    def partner(mask):
        a, r = flipped(me_a, mask // n_row), flipped(me_r, mask % n_row)
        return a * n_row + r, r, me_b * SPLIT + a

    masks = sorted(range(1, group), key=turns)
    partners = [partner(mask) for mask in masks]
    near_by = [partner(mask) for mask in masks if mask < plane]

    def earlier(mask):
        top = 1
        while 2 * top <= mask:
            top *= 2
        if top >= n_row:
            return lax.rem(lax.div(me_a, top // n_row), 2) == 1
        return lax.rem(lax.div(me_r, top), 2) == (0 if top == 1 else 1)

    steps = [1 << bit for bit in range(group.bit_length() - 1)]
    met = [
        (earlier(mask), *partner(mask)[1:], {n_row: 0, 2 * n_row: 1}.get(mask, 3))
        for mask in steps
    ]
    met += [(b < me_b, me_r, b * SPLIT + a, 2) for b in others for a in (me_a, far_a)]
    ahead = [earlier(n_row), earlier(2 * n_row)]
    barrier = pltpu.get_barrier_semaphore()
    for early_one, r, c, _ in met:

        @pl.when(jnp.logical_not(early_one))
        def _():
            pl.semaphore_signal(barrier, device_id={"prow": r, "pcol": c}, device_id_type=MESH)

    def count_of(kind, early_ones):
        flags = [m[0] if early_ones else jnp.logical_not(m[0]) for m in met if kind in (m[3], None)]
        return sum(flag.astype(jnp.int32) for flag in flags)

    def wait_for(sem, count):
        pl.when(count > 0)(lambda: pl.semaphore_wait(sem, count))

    def remote(src, dst, send, recv, r, c):
        return pltpu.make_async_remote_copy(
            src_ref=src, dst_ref=dst, send_sem=send, recv_sem=recv,
            device_id={"prow": r, "pcol": c}, device_id_type=MESH,
        )

    def wait(ref, sem):
        pltpu.make_async_copy(ref, ref, sem).wait()

    def cols_of(number):
        at, stop = pieces[number]
        return pl.ds(at, stop - at)

    def start(make, full, tail, q, number):
        at, stop = pieces[number]
        copy = make(full.at[..., pl.ds(pl.multiple_of(q * site + at, LANES), stop - at)])
        if at == main:
            pl.when(q == SPLIT - 1)(make(tail).start)
            pl.when(q != SPLIT - 1)(copy.start)
        else:
            copy.start()

    def v_slot(a):
        return lambda number: v_s.at[a, :, cols_of(number)]

    def w_slot(p, c):
        return lambda number: w_s.at[p, c, :, cols_of(number)]

    def v_half(number):
        return v_mid.at[:, cols_of(number)]

    def w_half(p):
        return lambda number: w_mid.at[p, :, cols_of(number)]

    def sent_of(p, number):
        return 0 if p else 1 if number < lent else 2

    def send_v(q, dst, come):
        def start_copy(number, c):
            start(
                lambda src: remote(src, dst(number), v_sent, come.at[number], me_r, c),
                v_ref, v_tail, q, number,
            )
        return start_copy

    def send_w(p, q, dst, come):
        def start_copy(number, c):
            start(
                lambda src: remote(src, dst(number), w_sent.at[sent_of(p, number)], come.at[p, number], me_r, c),
                w_ref.at[p], w_tail.at[p], q, number,
            )
        return start_copy

    def pass_v(src, dst):
        def start_copy(number, c):
            remote(src(number), dst(number), v_sent, v_came.at[number], me_r, c).start()
        return start_copy

    def pass_w(p, src, dst):
        def start_copy(number, c):
            remote(
                src(number), dst(number), w_sent.at[sent_of(p, number)], w_came.at[p, number], me_r, c
            ).start()
        return start_copy

    keep_t = pltpu.make_async_copy(t_ref, t_s, t_sem.at[0])
    keep_t.start()
    whole = [
        pltpu.make_async_copy(v_ref, v_all, t_sem.at[1]),
        pltpu.make_async_copy(w_ref, w_all, t_sem.at[2]),
    ]
    for copy in whole:
        copy.start()
    width = v_s.shape[2]
    if width > site:
        v_s[:, :, site:] = jnp.zeros((SPLIT, v_s.shape[1], width - site), BF16)
        w_s[:, :, :, site:] = jnp.zeros((2, n_col, w_s.shape[2], width - site), BF16)
    part[...] = jnp.zeros_like(part)
    wait_for(barrier, count_of(None, True))
    for early_one, r, c, kind in met:

        @pl.when(early_one)
        def _():
            pl.semaphore_signal(
                entered.at[kind], device_id={"prow": r, "pcol": c}, device_id_type=MESH
            )

    v_own = v_slot(me_a)
    near_v = send_v(far_a, v_own, v_came)
    near_v_on = pass_v(v_half, v_slot(side_a))
    stay, across, stay_on, across_on = [], [], [], []
    for p in range(2):
        w_own, w_other = w_slot(p, me_c), w_slot(p, side_c)
        stay.append(send_w(p, me_a, w_own, w_came))
        across.append(send_w(p, far_a, w_own, w_came))
        stay_on.append(pass_w(p, w_other, w_other))
        across_on.append(pass_w(p, w_half(p), w_other))

    def far(number, here, there):
        for b in others:
            there(number, b * SPLIT + far_a)
            here(number, b * SPLIT + me_a)

    to_lender = send_w(0, far_a, w_slot(0, me_c), lend_came)

    def near(number):
        near_v(number, far_c)
        if number < lent:
            pl.when(inner)(functools.partial(across[0], number, far_c))
            pl.when(jnp.logical_not(inner))(functools.partial(to_lender, number, far_c))
        else:
            across[0](number, far_c)

    def over(number, c):
        if number < lent:

            @pl.when(inner)
            def _():
                start(
                    lambda src: remote(
                        src, w_slot(0, me_c)(number), lend_sent, w_came.at[0, number], me_r, c
                    ),
                    w_ref.at[0], w_tail.at[0], far_a, number,
                )
        else:
            across[0](number, c)

    def to_earlier(number):
        for b in others:

            @pl.when(b < me_b)
            def _():
                over(number, b * SPLIT + far_a)
                stay[0](number, b * SPLIT + me_a)

        pl.when(ahead[1])(functools.partial(near, number))

    def to_later(number):
        for b in others:

            @pl.when(b > me_b)
            def _():
                over(number, b * SPLIT + far_a)
                stay[0](number, b * SPLIT + me_a)

        if number:
            pl.when(jnp.logical_not(ahead[1]))(functools.partial(near, number))

    def to_side(number):
        send_w(0, side_far, w_half(0), w_side)(number, side_c)
        send_v(side_far, v_half, v_side)(number, side_c)
        send_w(0, side_a, w_slot(0, me_c), w_side)(number, side_c)
        send_v(side_a, v_own, v_side)(number, side_c)

    for number in numbers[:-1]:
        to_earlier(number)
    wait_for(entered.at[0], count_of(0, False))
    for number in numbers[:-1]:
        to_side(number)
    wait_for(entered.at[1], count_of(1, False))
    pl.when(jnp.logical_not(ahead[1]))(functools.partial(near, 0))
    wait_for(entered.at[2], count_of(2, False))
    for number in numbers[:-1]:
        to_later(number)
    v_tail[...] = jnp.zeros_like(v_tail)
    w_tail[...] = jnp.zeros_like(w_tail)
    for copy in whole:
        copy.wait()
    if rest:
        edge = (SPLIT - 1) * site + main
        v_tail[:, :rest] = v_all[:, edge:edge + rest]
        w_tail[:, :, :rest] = w_all[:, :, edge:edge + rest]
    for send_last in (to_earlier, to_side, to_later):
        send_last(numbers[-1])
    for number in numbers:
        send_w(1, side_far, w_half(1), w_side)(number, side_c)
        send_w(1, side_a, w_slot(1, me_c), w_side)(number, side_c)

    @pl.when(inner)
    def _():
        for number in numbers:
            for b in others:
                across[1](number, b * SPLIT + far_a)

    for number in numbers:
        start(
            lambda src: pltpu.make_async_copy(src, v_own(number), l_sem.at[0]),
            v_ref, v_tail, me_a, number,
        )
        start(
            lambda src: pltpu.make_async_copy(src, w_s.at[:, me_c, :, cols_of(number)], l_sem.at[1]),
            w_ref, w_tail, me_a, number,
        )

    for number in numbers:
        wait(w_s.at[0, pl.ds(0, 2), :, cols_of(number)], w_side.at[0, number])
        wait(v_s.at[pl.ds(0, 2), :, cols_of(number)], v_side.at[number])
        far(number, stay_on[0], across_on[0])
        near_v_on(number, far_c)
        across_on[0](number, far_c)

    if lent:

        @pl.when(inner)
        def _():
            for number in numbers[:lent]:
                lend = w_slot(0, far_c)(number)
                wait(lend, lend_came.at[0, number])
                for b in others:
                    remote(
                        lend, lend, lend_sent, w_came.at[0, number], me_r, b * SPLIT + me_a
                    ).start()

    for number in numbers[:early]:

        @pl.when(jnp.logical_not(inner))
        def _():
            far(number, stay[1], across[1])

        across[1](number, far_c)
    for number in numbers:
        wait(w_s.at[1, pl.ds(0, 2), :, cols_of(number)], w_side.at[1, number])

        @pl.when(inner)
        def _():
            for b in others:
                across_on[1](number, b * SPLIT + far_a)

        if number < early:

            @pl.when(jnp.logical_not(inner))
            def _():
                far(number, stay_on[1], across_on[1])

            across_on[1](number, far_c)

    @pl.when(inner)
    def _():
        for number in numbers:
            for b in others:
                stay[1](number, b * SPLIT + me_a)
                stay_on[1](number, b * SPLIT + me_a)

    wait_for(entered.at[3], count_of(3, False))
    for k, mask in enumerate(steps):
        _, r, c = partner(mask)
        pl.semaphore_signal(told.at[k], device_id={"prow": r, "pcol": c}, device_id_type=MESH)
        pl.semaphore_wait(told.at[k], 1)

    def panel_of(p, cols):
        block = w_s[p, :, :, cols]
        if w_s.shape[2] % 16:
            block = block.astype(F32)
        return block.reshape(panel, block.shape[-1]).astype(BF16)

    def products(p, at, stop):
        cols = pl.ds(at, stop - at)
        v = v_s[:, :, cols].reshape(rows, stop - at)
        part[...] += lax.dot_general(v, panel_of(p, cols), NT, preferred_element_type=F32)

    def factor_of(p, sums):
        return lax.dot_general(
            sums, t_s[p], NT, precision=lax.Precision.HIGHEST, preferred_element_type=F32
        ).astype(BF16)

    def update(p, at, stop):
        @pl.loop(at // n_block, stop // n_block)
        def _(i):
            cols = pl.ds(pl.multiple_of(i * n_block, n_block), n_block)
            v = v_s[:, :, cols].reshape(rows, n_block).astype(F32)
            v = v - jnp.dot(s_s[...], panel_of(p, cols), preferred_element_type=F32)
            v_s[:, :, cols] = v.astype(BF16).reshape(SPLIT, rows // SPLIT, n_block)

    wait(v_s.at[0, :, pl.ds(0, site)], l_sem.at[0])
    wait(w_s.at[:, 0, :, pl.ds(0, site)], l_sem.at[1])
    for number in numbers:
        wait(v_s.at[pl.ds(0, 2), :, cols_of(number)], v_came.at[number])
        if number < lent:
            for own_role, slots in ((inner, n_col - 3), (jnp.logical_not(inner), n_col - 2)):
                pl.when(own_role)(functools.partial(
                    wait, w_s.at[0, pl.ds(0, slots), :, cols_of(number)], w_came.at[0, number]
                ))
        else:
            wait(w_s.at[0, pl.ds(0, n_col - 2), :, cols_of(number)], w_came.at[0, number])
        products(0, *sums_at[number])

    m_send[...] = part[...].reshape(m_send.shape)
    part[...] = jnp.zeros_like(part)
    for g, r, c in near_by:
        h = lax.rem(g, plane)
        remote(m_send.at[h], m_recv.at[me_h], m_sems.at[0], m_sems.at[1], r, c).start()
    m_recv[me_h] = m_send[me_h]
    wait(m_recv.at[pl.ds(0, plane - 1)], m_sems.at[1])
    z_send[...] = jnp.sum(m_recv[...], axis=0)
    remote(z_send, z_recv, m_sems.at[2], m_sems.at[3], me_r, far_c).start()
    for number in numbers[early:]:

        @pl.when(jnp.logical_not(inner))
        def _():
            far(number, stay[1], across[1])

        across[1](number, far_c)

        @pl.when(jnp.logical_not(inner))
        def _():
            far(number, stay_on[1], across_on[1])

        across_on[1](number, far_c)
    wait(z_recv, m_sems.at[3])
    m_all[me_h] = z_send[...] + z_recv[...]
    for _, r, c in near_by:
        remote(m_all.at[me_h], m_all.at[me_h], m_sems.at[4], m_sems.at[5], r, c).start()
    keep_t.wait()
    wait(m_all.at[pl.ds(0, plane - 1)], m_sems.at[5])
    s_s[...] = factor_of(0, m_all[...].reshape(rows, panel))
    update(0, 0, width)

    for number in numbers:
        wait(w_s.at[1, pl.ds(0, n_col - 2), :, cols_of(number)], w_came.at[1, number])
        products(1, *sums_at[number])

    rs_send[...] = part[...].astype(BF16).reshape(rs_send.shape)
    for g, r, c in partners:
        remote(rs_send.at[g], rs_recv.at[me_g], r_send, r_recv, r, c).start()
    rs_recv[me_g] = rs_send[me_g]
    wait(rs_recv.at[pl.ds(0, group - 1)], r_recv)
    ag[me_g] = factor_of(1, jnp.sum(rs_recv[...].astype(F32), axis=0))
    for g, r, c in partners:
        remote(ag.at[me_g], ag.at[me_g], g_send, g_recv, r, c).start()
    wait(ag.at[pl.ds(0, group - 1)], g_recv)
    s_s[...] = ag[...].reshape(rows, panel)

    def rows_of(r):
        return pl.ds(pl.multiple_of(r * own, own), own)

    for j, (at, stop) in enumerate(out_blocks):
        update(1, at, stop)
        cols = pl.ds(at, min(stop, site) - at)
        for g, r, c in partners:
            remote(
                v_s.at[lax.div(g, n_row), rows_of(r), cols], stage.at[me_g, :, cols],
                o_send, o_recv.at[j], r, c,
            ).start()

    for j, (at, stop) in enumerate(out_blocks):
        size = min(stop, site) - at
        cols = pl.ds(at, size)
        stage[me_g, :, cols] = v_s[me_a, rows_of(me_r), cols]
        wait(stage.at[pl.ds(0, group - 1), :, cols], o_recv.at[j])
        for r in range(n_row):
            for a in range(SPLIT):
                size = min(at + size, columns - a * site) - at
                begin = r * columns + a * site + at
                if size > 0:
                    o_ref[:, begin:begin + size] = stage[a * n_row + r, :, at:at + size]
                size = min(stop, site) - at
    wait(v_s.at[:, :, pl.ds(0, site)], v_sent)
    cut = pieces[lent][0]
    wait(w_s.at[1, :, :, pl.ds(0, site)], w_sent.at[0])
    if lent:
        wait(w_s.at[0, pl.ds(0, n_col - len(others)), :, pl.ds(0, cut)], w_sent.at[1])

        @pl.when(inner)
        def _():
            wait(w_s.at[0, pl.ds(0, 2 * len(others)), :, pl.ds(0, cut)], lend_sent)

    wait(w_s.at[0, :, :, pl.ds(cut, site - cut)], w_sent.at[2])
    wait(m_recv.at[pl.ds(0, plane - 1)], m_sems.at[0])
    wait(z_send, m_sems.at[2])
    wait(m_all.at[pl.ds(0, plane - 1)], m_sems.at[4])
    wait(rs_recv.at[pl.ds(0, group - 1)], r_send)
    wait(ag.at[pl.ds(0, group - 1)], g_send)
    wait(stage.at[pl.ds(0, group - 1)], o_send)


def body(n_row, n_col, vectors, reflectors, panel_factor):
    own_rows, columns = vectors.shape
    part_rows, panel = reflectors.shape[1], panel_factor.shape[1]
    group, plane, rows = SPLIT * n_row, 2 * n_row, SPLIT * own_rows
    site = -(-columns // (SPLIT * LANES)) * LANES
    last = columns - (SPLIT - 1) * site
    main, rest = last // LANES * LANES, last % LANES
    n_block = 2 * LANES
    width = -(-site // n_block) * n_block
    step = -(-main // (4 * n_block)) * n_block
    cuts = list(range(0, main, step)) + [main]
    even = main // n_block * n_block
    pieces = tuple(zip(cuts[:-1], cuts[1:])) + ((main, site),)
    sums_at = tuple((s, min(e, even)) for s, e in pieces[:-1]) + ((even, width),)
    marks = [0, 2 * n_block]
    blocks = width // n_block
    marks += [n_block * (2 + (blocks - 2) * k // 6) for k in range(1, 7)]
    out_blocks = tuple(zip(marks[:-1], marks[1:]))
    count = len(pieces)
    dma = pltpu.SemaphoreType.DMA
    plan = (site, main, rest, pieces, sums_at, out_blocks, n_block, 2, 2)
    whole = pl.pallas_call(
        functools.partial(kernel, n_row, n_col, columns, plan),
        out_shape=jax.ShapeDtypeStruct((own_rows // n_row, n_row * columns), BF16),
        in_specs=[
            pl.BlockSpec(memory_space=pl.ANY),
            pl.BlockSpec(memory_space=pl.ANY),
            pl.BlockSpec(memory_space=pltpu.HBM),
        ],
        out_specs=pl.BlockSpec(memory_space=pltpu.VMEM),
        scratch_shapes=[
            pltpu.VMEM((SPLIT, own_rows, width), BF16),
            pltpu.VMEM((2, n_col, part_rows, width), BF16),
            pltpu.VMEM((own_rows, site), BF16),
            pltpu.VMEM((2, part_rows, site), BF16),
            pltpu.VMEM((own_rows, site - main), BF16),
            pltpu.VMEM((2, part_rows, site - main), BF16),
            pltpu.VMEM(vectors.shape, BF16),
            pltpu.VMEM(reflectors.shape, BF16),
            pltpu.VMEM(panel_factor.shape, F32),
            pltpu.VMEM((rows, panel), F32),
            pltpu.VMEM((rows, panel), BF16),
            pltpu.VMEM((group, own_rows // n_row, site), BF16),
            pltpu.VMEM((plane, rows // plane, panel), F32),
            pltpu.VMEM((plane, rows // plane, panel), F32),
            pltpu.VMEM((rows // plane, panel), F32),
            pltpu.VMEM((rows // plane, panel), F32),
            pltpu.VMEM((plane, rows // plane, panel), F32),
            pltpu.VMEM((group, rows // group, panel), BF16),
            pltpu.VMEM((group, rows // group, panel), BF16),
            pltpu.VMEM((group, rows // group, panel), BF16),
            dma, dma((3,)), dma((count,)), dma((2, count)), dma((count,)), dma((2, count)), dma((2,)), dma((3,)),
            dma, dma((1, count)),
            dma((6,)), dma, dma, dma, dma, dma, dma((len(out_blocks),)),
            pltpu.SemaphoreType.REGULAR((4,)),
            pltpu.SemaphoreType.REGULAR((group.bit_length() - 1,)),
        ],
        compiler_params=pltpu.CompilerParams(
            has_side_effects=True, collective_id=0, vmem_limit_bytes=48 * 1024 * 1024
        ),
        name="panels",
    )(
        vectors, reflectors,
        pltpu.with_memory_space_constraint(panel_factor, pltpu.HBM),
    )
    return whole[None]


def solution(mesh):
    placed = (P("pcol", "prow"), P(None, "pcol", "prow"), P())
    return jax.shard_map(
        functools.partial(body, mesh.shape["prow"], mesh.shape["pcol"]),
        mesh=mesh, in_specs=placed, out_specs=P("pcol", "prow", None), check_vma=False,
    )
```

```python
import functools

import jax
import jax.numpy as jnp
from jax import lax
from jax.experimental import pallas as pl
from jax.experimental.pallas import tpu as pltpu
from jax.sharding import PartitionSpec as P

MESH = pl.DeviceIdType.MESH
LANES = 128
SPLIT = 4
F32, BF16 = jnp.float32, jnp.bfloat16
NT = (((1,), (1,)), ((), ()))


def flip(index, bit):
    return index + bit - 2 * bit * lax.rem(lax.div(index, bit), 2)


def flipped(index, mask):
    bit = 1
    while bit <= mask:
        if mask & bit:
            index = flip(index, bit)
        bit *= 2
    return index


def kernel(
    n_row, n_col, columns, plan,
    v_ref, w_ref, t_ref, o_ref,
    v_s, w_s, v_mid, w_mid, v_tail, w_tail, v_all, w_all, t_s, part, s_s, stage,
    m_send, m_recv, z_send, z_recv, m_all, rs_send, rs_recv, ag,
    v_sent, w_sent, v_came, w_came, v_side, w_side, l_sem, t_sem, lend_sent, lend_came,
    m_sems, r_send, r_recv, g_send, g_recv, o_send, o_recv, entered, told,
):
    site, main, rest, pieces, sums_at, out_blocks, n_block, early, lent = plan
    me_r, me_c = lax.axis_index("prow"), lax.axis_index("pcol")
    me_a, me_b = lax.rem(me_c, SPLIT), lax.div(me_c, SPLIT)
    me_x, me_e = lax.rem(me_a, 2), lax.div(me_a, 2)
    halves, group, plane = n_col // SPLIT, SPLIT * n_row, 2 * n_row
    me_g, me_h = me_a * n_row + me_r, me_x * n_row + me_r
    inner = lax.rem(me_b + me_e, 2) == 1
    rows = SPLIT * v_s.shape[1]
    panel = w_s.shape[1] * w_s.shape[2]
    own = v_s.shape[1] // n_row
    side_c, side_a = flip(me_c, 1), flip(me_a, 1)
    far_a, side_far = flip(me_a, 2), flip(side_a, 2)
    far_c = me_b * SPLIT + far_a
    others = [lax.rem(me_b + k, halves) for k in range(1, halves)]
    numbers = range(len(pieces))

    def turns(mask):
        a, r = mask // n_row, mask % n_row
        first = 0 if a & 2 else 1 if a & 1 else 2 if r > 1 else 3
        size = -(bool(a & 1) * 2 + (r > 1)) if first == 0 else (r > 1)
        return first, size, mask

    def partner(mask):
        a, r = flipped(me_a, mask // n_row), flipped(me_r, mask % n_row)
        return a * n_row + r, r, me_b * SPLIT + a

    masks = sorted(range(1, group), key=turns)
    partners = [partner(mask) for mask in masks]
    near_by = [partner(mask) for mask in masks if mask < plane]

    def earlier(mask):
        top = 1
        while 2 * top <= mask:
            top *= 2
        if top >= n_row:
            return lax.rem(lax.div(me_a, top // n_row), 2) == 1
        return lax.rem(lax.div(me_r, top), 2) == (0 if top == 1 else 1)

    steps = [1 << bit for bit in range(group.bit_length() - 1)]
    met = [
        (earlier(mask), *partner(mask)[1:], {n_row: 0, 2 * n_row: 1}.get(mask, 3))
        for mask in steps
    ]
    met += [(b < me_b, me_r, b * SPLIT + me_a, 2) for b in others]
    met += [(b < me_b, me_r, b * SPLIT + far_a, 4) for b in others]
    ahead = [earlier(n_row), earlier(2 * n_row)]
    barrier = pltpu.get_barrier_semaphore()
    for early_one, r, c, _ in met:

        @pl.when(jnp.logical_not(early_one))
        def _():
            pl.semaphore_signal(barrier, device_id={"prow": r, "pcol": c}, device_id_type=MESH)

    def count_of(kind, early_ones):
        flags = [m[0] if early_ones else jnp.logical_not(m[0]) for m in met if kind in (m[3], None)]
        return sum(flag.astype(jnp.int32) for flag in flags)

    def wait_for(sem, count):
        pl.when(count > 0)(lambda: pl.semaphore_wait(sem, count))

    def remote(src, dst, send, recv, r, c):
        return pltpu.make_async_remote_copy(
            src_ref=src, dst_ref=dst, send_sem=send, recv_sem=recv,
            device_id={"prow": r, "pcol": c}, device_id_type=MESH,
        )

    def wait(ref, sem):
        pltpu.make_async_copy(ref, ref, sem).wait()

    def cols_of(number):
        at, stop = pieces[number]
        return pl.ds(at, stop - at)

    def start(make, full, tail, q, number):
        at, stop = pieces[number]
        copy = make(full.at[..., pl.ds(pl.multiple_of(q * site + at, LANES), stop - at)])
        if at == main:
            pl.when(q == SPLIT - 1)(make(tail).start)
            pl.when(q != SPLIT - 1)(copy.start)
        else:
            copy.start()

    def v_slot(a):
        return lambda number: v_s.at[a, :, cols_of(number)]

    def w_slot(p, c):
        return lambda number: w_s.at[p, c, :, cols_of(number)]

    def v_half(number):
        return v_mid.at[:, cols_of(number)]

    def w_half(p):
        return lambda number: w_mid.at[p, :, cols_of(number)]

    def sent_of(p, number):
        return 0 if p else 1 if number < lent else 2

    def send_v(q, dst, come):
        def start_copy(number, c):
            start(
                lambda src: remote(src, dst(number), v_sent, come.at[number], me_r, c),
                v_ref, v_tail, q, number,
            )
        return start_copy

    def send_w(p, q, dst, come):
        def start_copy(number, c):
            start(
                lambda src: remote(src, dst(number), w_sent.at[sent_of(p, number)], come.at[p, number], me_r, c),
                w_ref.at[p], w_tail.at[p], q, number,
            )
        return start_copy

    def pass_v(src, dst):
        def start_copy(number, c):
            remote(src(number), dst(number), v_sent, v_came.at[number], me_r, c).start()
        return start_copy

    def pass_w(p, src, dst):
        def start_copy(number, c):
            remote(
                src(number), dst(number), w_sent.at[sent_of(p, number)], w_came.at[p, number], me_r, c
            ).start()
        return start_copy

    keep_t = pltpu.make_async_copy(t_ref, t_s, t_sem.at[0])
    keep_t.start()
    whole = [
        pltpu.make_async_copy(v_ref, v_all, t_sem.at[1]),
        pltpu.make_async_copy(w_ref, w_all, t_sem.at[2]),
    ]
    for copy in whole:
        copy.start()
    width = v_s.shape[2]
    if width > site:
        v_s[:, :, site:] = jnp.zeros((SPLIT, v_s.shape[1], width - site), BF16)
        w_s[:, :, :, site:] = jnp.zeros((2, n_col, w_s.shape[2], width - site), BF16)
    part[...] = jnp.zeros_like(part)
    wait_for(barrier, count_of(None, True))
    for early_one, r, c, kind in met:

        @pl.when(early_one)
        def _():
            pl.semaphore_signal(
                entered.at[kind], device_id={"prow": r, "pcol": c}, device_id_type=MESH
            )

    v_own = v_slot(me_a)
    near_v = send_v(far_a, v_own, v_came)
    near_v_on = pass_v(v_half, v_slot(side_a))
    stay, across, stay_on, across_on = [], [], [], []
    for p in range(2):
        w_own, w_other = w_slot(p, me_c), w_slot(p, side_c)
        stay.append(send_w(p, me_a, w_own, w_came))
        across.append(send_w(p, far_a, w_own, w_came))
        stay_on.append(pass_w(p, w_other, w_other))
        across_on.append(pass_w(p, w_half(p), w_other))

    def far(number, here, there):
        for b in others:
            there(number, b * SPLIT + far_a)
            here(number, b * SPLIT + me_a)

    to_lender = send_w(0, far_a, w_slot(0, me_c), lend_came)

    def near(number):
        near_v(number, far_c)
        if number < lent:
            pl.when(inner)(functools.partial(across[0], number, far_c))
            pl.when(jnp.logical_not(inner))(functools.partial(to_lender, number, far_c))
        else:
            across[0](number, far_c)

    def over(number, c):
        if number < lent:

            @pl.when(inner)
            def _():
                start(
                    lambda src: remote(
                        src, w_slot(0, me_c)(number), lend_sent, w_came.at[0, number], me_r, c
                    ),
                    w_ref.at[0], w_tail.at[0], far_a, number,
                )
        else:
            across[0](number, c)

    def to_earlier(number):
        for b in others:

            @pl.when(b < me_b)
            def _():
                over(number, b * SPLIT + far_a)
                stay[0](number, b * SPLIT + me_a)

        pl.when(ahead[1])(functools.partial(near, number))

    def to_later(number):
        for b in others:

            @pl.when(b > me_b)
            def _():
                if number:
                    over(number, b * SPLIT + far_a)
                else:
                    pl.when(jnp.logical_not(inner))(
                        functools.partial(over, 0, b * SPLIT + far_a)
                    )
                stay[0](number, b * SPLIT + me_a)

        if number:
            pl.when(jnp.logical_not(ahead[1]))(functools.partial(near, number))

    def to_side(number):
        send_w(0, side_far, w_half(0), w_side)(number, side_c)
        send_v(side_far, v_half, v_side)(number, side_c)
        send_w(0, side_a, w_slot(0, me_c), w_side)(number, side_c)
        send_v(side_a, v_own, v_side)(number, side_c)

    for number in numbers[:-1]:
        to_earlier(number)
    wait_for(entered.at[0], count_of(0, False))
    for number in numbers[:-1]:
        to_side(number)
    wait_for(entered.at[1], count_of(1, False))
    pl.when(jnp.logical_not(ahead[1]))(functools.partial(near, 0))
    wait_for(entered.at[4], count_of(4, False))
    for b in others:
        pl.when(inner & (b > me_b))(functools.partial(over, 0, b * SPLIT + far_a))
    wait_for(entered.at[2], count_of(2, False))
    for number in numbers[:-1]:
        to_later(number)
    v_tail[...] = jnp.zeros_like(v_tail)
    w_tail[...] = jnp.zeros_like(w_tail)
    for copy in whole:
        copy.wait()
    if rest:
        edge = (SPLIT - 1) * site + main
        v_tail[:, :rest] = v_all[:, edge:edge + rest]
        w_tail[:, :, :rest] = w_all[:, :, edge:edge + rest]
    for send_last in (to_earlier, to_side, to_later):
        send_last(numbers[-1])
    for number in numbers:
        send_w(1, side_far, w_half(1), w_side)(number, side_c)
        send_w(1, side_a, w_slot(1, me_c), w_side)(number, side_c)

    @pl.when(inner)
    def _():
        for number in numbers:
            for b in others:
                across[1](number, b * SPLIT + far_a)

    for number in numbers:
        start(
            lambda src: pltpu.make_async_copy(src, v_own(number), l_sem.at[0]),
            v_ref, v_tail, me_a, number,
        )
        start(
            lambda src: pltpu.make_async_copy(src, w_s.at[:, me_c, :, cols_of(number)], l_sem.at[1]),
            w_ref, w_tail, me_a, number,
        )

    for number in numbers:
        wait(w_s.at[0, pl.ds(0, 2), :, cols_of(number)], w_side.at[0, number])
        wait(v_s.at[pl.ds(0, 2), :, cols_of(number)], v_side.at[number])
        far(number, stay_on[0], across_on[0])
        near_v_on(number, far_c)
        across_on[0](number, far_c)

    if lent:

        @pl.when(inner)
        def _():
            for number in numbers[:lent]:
                lend = w_slot(0, far_c)(number)
                wait(lend, lend_came.at[0, number])
                for b in others:
                    remote(
                        lend, lend, lend_sent, w_came.at[0, number], me_r, b * SPLIT + me_a
                    ).start()

    for number in numbers[:early]:

        @pl.when(jnp.logical_not(inner))
        def _():
            far(number, stay[1], across[1])

        across[1](number, far_c)
    for number in numbers:
        wait(w_s.at[1, pl.ds(0, 2), :, cols_of(number)], w_side.at[1, number])

        if number < 3:

            @pl.when(inner)
            def _():
                for b in others:
                    across_on[1](number, b * SPLIT + far_a)

        if number < early:

            @pl.when(jnp.logical_not(inner))
            def _():
                far(number, stay_on[1], across_on[1])

            across_on[1](number, far_c)

    @pl.when(inner)
    def _():
        for number in numbers:
            for b in others:
                stay[1](number, b * SPLIT + me_a)
                stay_on[1](number, b * SPLIT + me_a)
        for number in numbers[3:]:
            for b in others:
                across_on[1](number, b * SPLIT + far_a)

    wait_for(entered.at[3], count_of(3, False))
    for k, mask in enumerate(steps):
        _, r, c = partner(mask)
        pl.semaphore_signal(told.at[k], device_id={"prow": r, "pcol": c}, device_id_type=MESH)
        pl.semaphore_wait(told.at[k], 1)

    def panel_of(p, cols):
        block = w_s[p, :, :, cols]
        if w_s.shape[2] % 16:
            block = block.astype(F32)
        return block.reshape(panel, block.shape[-1]).astype(BF16)

    def products(p, at, stop):
        cols = pl.ds(at, stop - at)
        v = v_s[:, :, cols].reshape(rows, stop - at)
        part[...] += lax.dot_general(v, panel_of(p, cols), NT, preferred_element_type=F32)

    def factor_of(p, sums):
        return lax.dot_general(
            sums, t_s[p], NT, precision=lax.Precision.HIGHEST, preferred_element_type=F32
        ).astype(BF16)

    def update(p, at, stop):
        @pl.loop(at // n_block, stop // n_block)
        def _(i):
            cols = pl.ds(pl.multiple_of(i * n_block, n_block), n_block)
            v = v_s[:, :, cols].reshape(rows, n_block).astype(F32)
            v = v - jnp.dot(s_s[...], panel_of(p, cols), preferred_element_type=F32)
            v_s[:, :, cols] = v.astype(BF16).reshape(SPLIT, rows // SPLIT, n_block)

    wait(v_s.at[0, :, pl.ds(0, site)], l_sem.at[0])
    wait(w_s.at[:, 0, :, pl.ds(0, site)], l_sem.at[1])
    for number in numbers:
        wait(v_s.at[pl.ds(0, 2), :, cols_of(number)], v_came.at[number])
        if number < lent:
            for own_role, slots in ((inner, n_col - 3), (jnp.logical_not(inner), n_col - 2)):
                pl.when(own_role)(functools.partial(
                    wait, w_s.at[0, pl.ds(0, slots), :, cols_of(number)], w_came.at[0, number]
                ))
        else:
            wait(w_s.at[0, pl.ds(0, n_col - 2), :, cols_of(number)], w_came.at[0, number])
        products(0, *sums_at[number])

    m_send[...] = part[...].reshape(m_send.shape)
    part[...] = jnp.zeros_like(part)
    for g, r, c in near_by:
        h = lax.rem(g, plane)
        remote(m_send.at[h], m_recv.at[me_h], m_sems.at[0], m_sems.at[1], r, c).start()
    m_recv[me_h] = m_send[me_h]
    wait(m_recv.at[pl.ds(0, plane - 1)], m_sems.at[1])
    z_send[...] = jnp.sum(m_recv[...], axis=0)
    remote(z_send, z_recv, m_sems.at[2], m_sems.at[3], me_r, far_c).start()
    for number in numbers[early:]:

        @pl.when(jnp.logical_not(inner))
        def _():
            far(number, stay[1], across[1])

        across[1](number, far_c)

        @pl.when(jnp.logical_not(inner))
        def _():
            far(number, stay_on[1], across_on[1])

        across_on[1](number, far_c)
    wait(z_recv, m_sems.at[3])
    m_all[me_h] = z_send[...] + z_recv[...]
    for _, r, c in near_by:
        remote(m_all.at[me_h], m_all.at[me_h], m_sems.at[4], m_sems.at[5], r, c).start()
    keep_t.wait()
    wait(m_all.at[pl.ds(0, plane - 1)], m_sems.at[5])
    s_s[...] = factor_of(0, m_all[...].reshape(rows, panel))
    update(0, 0, width)

    for number in numbers:
        wait(w_s.at[1, pl.ds(0, n_col - 2), :, cols_of(number)], w_came.at[1, number])
        products(1, *sums_at[number])

    rs_send[...] = part[...].astype(BF16).reshape(rs_send.shape)
    for g, r, c in partners:
        remote(rs_send.at[g], rs_recv.at[me_g], r_send, r_recv, r, c).start()
    rs_recv[me_g] = rs_send[me_g]
    wait(rs_recv.at[pl.ds(0, group - 1)], r_recv)
    ag[me_g] = factor_of(1, jnp.sum(rs_recv[...].astype(F32), axis=0))
    for g, r, c in partners:
        remote(ag.at[me_g], ag.at[me_g], g_send, g_recv, r, c).start()
    wait(ag.at[pl.ds(0, group - 1)], g_recv)
    s_s[...] = ag[...].reshape(rows, panel)

    def rows_of(r):
        return pl.ds(pl.multiple_of(r * own, own), own)

    for j, (at, stop) in enumerate(out_blocks):
        update(1, at, stop)
        cols = pl.ds(at, min(stop, site) - at)
        for g, r, c in partners:
            remote(
                v_s.at[lax.div(g, n_row), rows_of(r), cols], stage.at[me_g, :, cols],
                o_send, o_recv.at[j], r, c,
            ).start()

    for j, (at, stop) in enumerate(out_blocks):
        size = min(stop, site) - at
        cols = pl.ds(at, size)
        stage[me_g, :, cols] = v_s[me_a, rows_of(me_r), cols]
        wait(stage.at[pl.ds(0, group - 1), :, cols], o_recv.at[j])
        for r in range(n_row):
            for a in range(SPLIT):
                size = min(at + size, columns - a * site) - at
                begin = r * columns + a * site + at
                if size > 0:
                    o_ref[:, begin:begin + size] = stage[a * n_row + r, :, at:at + size]
                size = min(stop, site) - at
    wait(v_s.at[:, :, pl.ds(0, site)], v_sent)
    cut = pieces[lent][0]
    wait(w_s.at[1, :, :, pl.ds(0, site)], w_sent.at[0])
    if lent:
        wait(w_s.at[0, pl.ds(0, n_col - len(others)), :, pl.ds(0, cut)], w_sent.at[1])

        @pl.when(inner)
        def _():
            wait(w_s.at[0, pl.ds(0, 2 * len(others)), :, pl.ds(0, cut)], lend_sent)

    wait(w_s.at[0, :, :, pl.ds(cut, site - cut)], w_sent.at[2])
    wait(m_recv.at[pl.ds(0, plane - 1)], m_sems.at[0])
    wait(z_send, m_sems.at[2])
    wait(m_all.at[pl.ds(0, plane - 1)], m_sems.at[4])
    wait(rs_recv.at[pl.ds(0, group - 1)], r_send)
    wait(ag.at[pl.ds(0, group - 1)], g_send)
    wait(stage.at[pl.ds(0, group - 1)], o_send)


def body(n_row, n_col, vectors, reflectors, panel_factor):
    own_rows, columns = vectors.shape
    part_rows, panel = reflectors.shape[1], panel_factor.shape[1]
    group, plane, rows = SPLIT * n_row, 2 * n_row, SPLIT * own_rows
    site = -(-columns // (SPLIT * LANES)) * LANES
    last = columns - (SPLIT - 1) * site
    main, rest = last // LANES * LANES, last % LANES
    n_block = 2 * LANES
    width = -(-site // n_block) * n_block
    step = -(-main // (4 * n_block)) * n_block
    cuts = list(range(0, main, step)) + [main]
    even = main // n_block * n_block
    pieces = tuple(zip(cuts[:-1], cuts[1:])) + ((main, site),)
    sums_at = tuple((s, min(e, even)) for s, e in pieces[:-1]) + ((even, width),)
    marks = [0, 2 * n_block]
    blocks = width // n_block
    marks += [n_block * (2 + (blocks - 2) * k // 6) for k in range(1, 7)]
    out_blocks = tuple(zip(marks[:-1], marks[1:]))
    count = len(pieces)
    dma = pltpu.SemaphoreType.DMA
    plan = (site, main, rest, pieces, sums_at, out_blocks, n_block, 2, 2)
    whole = pl.pallas_call(
        functools.partial(kernel, n_row, n_col, columns, plan),
        out_shape=jax.ShapeDtypeStruct((own_rows // n_row, n_row * columns), BF16),
        in_specs=[
            pl.BlockSpec(memory_space=pl.ANY),
            pl.BlockSpec(memory_space=pl.ANY),
            pl.BlockSpec(memory_space=pltpu.HBM),
        ],
        out_specs=pl.BlockSpec(memory_space=pltpu.VMEM),
        scratch_shapes=[
            pltpu.VMEM((SPLIT, own_rows, width), BF16),
            pltpu.VMEM((2, n_col, part_rows, width), BF16),
            pltpu.VMEM((own_rows, site), BF16),
            pltpu.VMEM((2, part_rows, site), BF16),
            pltpu.VMEM((own_rows, site - main), BF16),
            pltpu.VMEM((2, part_rows, site - main), BF16),
            pltpu.VMEM(vectors.shape, BF16),
            pltpu.VMEM(reflectors.shape, BF16),
            pltpu.VMEM(panel_factor.shape, F32),
            pltpu.VMEM((rows, panel), F32),
            pltpu.VMEM((rows, panel), BF16),
            pltpu.VMEM((group, own_rows // n_row, site), BF16),
            pltpu.VMEM((plane, rows // plane, panel), F32),
            pltpu.VMEM((plane, rows // plane, panel), F32),
            pltpu.VMEM((rows // plane, panel), F32),
            pltpu.VMEM((rows // plane, panel), F32),
            pltpu.VMEM((plane, rows // plane, panel), F32),
            pltpu.VMEM((group, rows // group, panel), BF16),
            pltpu.VMEM((group, rows // group, panel), BF16),
            pltpu.VMEM((group, rows // group, panel), BF16),
            dma, dma((3,)), dma((count,)), dma((2, count)), dma((count,)), dma((2, count)), dma((2,)), dma((3,)),
            dma, dma((1, count)),
            dma((6,)), dma, dma, dma, dma, dma, dma((len(out_blocks),)),
            pltpu.SemaphoreType.REGULAR((5,)),
            pltpu.SemaphoreType.REGULAR((group.bit_length() - 1,)),
        ],
        compiler_params=pltpu.CompilerParams(
            has_side_effects=True, collective_id=0, vmem_limit_bytes=48 * 1024 * 1024
        ),
        name="panels",
    )(
        vectors, reflectors,
        pltpu.with_memory_space_constraint(panel_factor, pltpu.HBM),
    )
    return whole[None]


def solution(mesh):
    placed = (P("pcol", "prow"), P(None, "pcol", "prow"), P())
    return jax.shard_map(
        functools.partial(body, mesh.shape["prow"], mesh.shape["pcol"]),
        mesh=mesh, in_specs=placed, out_specs=P("pcol", "prow", None), check_vma=False,
    )
```

```python
import functools

import jax
import jax.numpy as jnp
from jax import lax
from jax.experimental import pallas as pl
from jax.experimental.pallas import tpu as pltpu
from jax.sharding import PartitionSpec as P

MESH = pl.DeviceIdType.MESH
LANES = 128
SPLIT = 4
F32, BF16 = jnp.float32, jnp.bfloat16
NT = (((1,), (1,)), ((), ()))


def flip(index, bit):
    return index + bit - 2 * bit * lax.rem(lax.div(index, bit), 2)


def flipped(index, mask):
    bit = 1
    while bit <= mask:
        if mask & bit:
            index = flip(index, bit)
        bit *= 2
    return index


def kernel(
    n_row, n_col, columns, plan,
    v_ref, w_ref, t_ref, o_ref,
    v_s, w_s, v_mid, w_mid, v_tail, w_tail, v_all, w_all, t_s, part, s_s, stage,
    m_send, m_recv, z_send, z_recv, m_all, rs_send, rs_recv, ag,
    v_sent, w_sent, v_came, w_came, v_side, w_side, l_sem, t_sem, lend_sent, lend_came,
    m_sems, r_send, r_recv, g_send, g_recv, o_send, o_recv, entered, told,
):
    site, main, rest, pieces, sums_at, out_blocks, n_block, early, lent = plan
    me_r, me_c = lax.axis_index("prow"), lax.axis_index("pcol")
    me_a, me_b = lax.rem(me_c, SPLIT), lax.div(me_c, SPLIT)
    me_x, me_e = lax.rem(me_a, 2), lax.div(me_a, 2)
    halves, group, plane = n_col // SPLIT, SPLIT * n_row, 2 * n_row
    me_g, me_h = me_a * n_row + me_r, me_x * n_row + me_r
    inner = lax.rem(me_b + me_e, 2) == 1
    rows = SPLIT * v_s.shape[1]
    panel = w_s.shape[1] * w_s.shape[2]
    own = v_s.shape[1] // n_row
    side_c, side_a = flip(me_c, 1), flip(me_a, 1)
    far_a, side_far = flip(me_a, 2), flip(side_a, 2)
    far_c = me_b * SPLIT + far_a
    others = [lax.rem(me_b + k, halves) for k in range(1, halves)]
    numbers = range(len(pieces))

    def turns(mask):
        a, r = mask // n_row, mask % n_row
        first = 0 if a & 2 else 1 if a & 1 else 2 if r > 1 else 3
        size = -(bool(a & 1) * 2 + (r > 1)) if first == 0 else (r > 1)
        return first, size, mask

    def partner(mask):
        a, r = flipped(me_a, mask // n_row), flipped(me_r, mask % n_row)
        return a * n_row + r, r, me_b * SPLIT + a

    masks = sorted(range(1, group), key=turns)
    partners = [partner(mask) for mask in masks]
    near_by = [partner(mask) for mask in masks if mask < plane]

    def earlier(mask):
        top = 1
        while 2 * top <= mask:
            top *= 2
        if top >= n_row:
            return lax.rem(lax.div(me_a, top // n_row), 2) == 1
        return lax.rem(lax.div(me_r, top), 2) == (0 if top == 1 else 1)

    steps = [1 << bit for bit in range(group.bit_length() - 1)]
    met = [
        (earlier(mask), *partner(mask)[1:], {n_row: 0, 2 * n_row: 1}.get(mask, 3))
        for mask in steps
    ]
    met += [(b < me_b, me_r, b * SPLIT + a, 2) for b in others for a in (me_a, far_a)]
    ahead = [earlier(n_row), earlier(2 * n_row)]
    barrier = pltpu.get_barrier_semaphore()
    for early_one, r, c, _ in met:

        @pl.when(jnp.logical_not(early_one))
        def _():
            pl.semaphore_signal(barrier, device_id={"prow": r, "pcol": c}, device_id_type=MESH)

    def count_of(kind, early_ones):
        flags = [m[0] if early_ones else jnp.logical_not(m[0]) for m in met if kind in (m[3], None)]
        return sum(flag.astype(jnp.int32) for flag in flags)

    def wait_for(sem, count):
        pl.when(count > 0)(lambda: pl.semaphore_wait(sem, count))

    def remote(src, dst, send, recv, r, c):
        return pltpu.make_async_remote_copy(
            src_ref=src, dst_ref=dst, send_sem=send, recv_sem=recv,
            device_id={"prow": r, "pcol": c}, device_id_type=MESH,
        )

    def wait(ref, sem):
        pltpu.make_async_copy(ref, ref, sem).wait()

    def cols_of(number):
        at, stop = pieces[number]
        return pl.ds(at, stop - at)

    def start(make, full, tail, q, number):
        at, stop = pieces[number]
        copy = make(full.at[..., pl.ds(pl.multiple_of(q * site + at, LANES), stop - at)])
        if at == main:
            pl.when(q == SPLIT - 1)(make(tail).start)
            pl.when(q != SPLIT - 1)(copy.start)
        else:
            copy.start()

    def v_slot(a):
        return lambda number: v_s.at[a, :, cols_of(number)]

    def w_slot(p, c):
        return lambda number: w_s.at[p, c, :, cols_of(number)]

    def v_half(number):
        return v_mid.at[:, cols_of(number)]

    def w_half(p):
        return lambda number: w_mid.at[p, :, cols_of(number)]

    def sent_of(p, number):
        return 0 if p else 1 if number < lent else 2

    def send_v(q, dst, come):
        def start_copy(number, c):
            start(
                lambda src: remote(src, dst(number), v_sent, come.at[number], me_r, c),
                v_ref, v_tail, q, number,
            )
        return start_copy

    def send_w(p, q, dst, come):
        def start_copy(number, c):
            start(
                lambda src: remote(src, dst(number), w_sent.at[sent_of(p, number)], come.at[p, number], me_r, c),
                w_ref.at[p], w_tail.at[p], q, number,
            )
        return start_copy

    def pass_v(src, dst):
        def start_copy(number, c):
            remote(src(number), dst(number), v_sent, v_came.at[number], me_r, c).start()
        return start_copy

    def pass_w(p, src, dst):
        def start_copy(number, c):
            remote(
                src(number), dst(number), w_sent.at[sent_of(p, number)], w_came.at[p, number], me_r, c
            ).start()
        return start_copy

    keep_t = pltpu.make_async_copy(t_ref, t_s, t_sem.at[0])
    keep_t.start()
    whole = [
        pltpu.make_async_copy(v_ref, v_all, t_sem.at[1]),
        pltpu.make_async_copy(w_ref, w_all, t_sem.at[2]),
    ]
    for copy in whole:
        copy.start()
    width = v_s.shape[2]
    if width > site:
        v_s[:, :, site:] = jnp.zeros((SPLIT, v_s.shape[1], width - site), BF16)
        w_s[:, :, :, site:] = jnp.zeros((2, n_col, w_s.shape[2], width - site), BF16)
    part[...] = jnp.zeros_like(part)
    wait_for(barrier, count_of(None, True))
    for early_one, r, c, kind in met:

        @pl.when(early_one)
        def _():
            pl.semaphore_signal(
                entered.at[kind], device_id={"prow": r, "pcol": c}, device_id_type=MESH
            )

    v_own = v_slot(me_a)
    near_v = send_v(far_a, v_own, v_came)
    near_v_on = pass_v(v_half, v_slot(side_a))
    stay, across, stay_on, across_on = [], [], [], []
    for p in range(2):
        w_own, w_other = w_slot(p, me_c), w_slot(p, side_c)
        stay.append(send_w(p, me_a, w_own, w_came))
        across.append(send_w(p, far_a, w_own, w_came))
        stay_on.append(pass_w(p, w_other, w_other))
        across_on.append(pass_w(p, w_half(p), w_other))

    def far(number, here, there):
        for b in others:
            there(number, b * SPLIT + far_a)
            here(number, b * SPLIT + me_a)

    to_lender = send_w(0, far_a, w_slot(0, me_c), lend_came)

    def near(number):
        near_v(number, far_c)
        if number < lent:
            pl.when(inner)(functools.partial(across[0], number, far_c))
            pl.when(jnp.logical_not(inner))(functools.partial(to_lender, number, far_c))
        else:
            across[0](number, far_c)

    def over(number, c):
        if number < lent:

            @pl.when(inner)
            def _():
                start(
                    lambda src: remote(
                        src, w_slot(0, me_c)(number), lend_sent, w_came.at[0, number], me_r, c
                    ),
                    w_ref.at[0], w_tail.at[0], far_a, number,
                )
        else:
            across[0](number, c)

    def to_earlier(number):
        for b in others:

            @pl.when(b < me_b)
            def _():
                over(number, b * SPLIT + far_a)
                stay[0](number, b * SPLIT + me_a)

        pl.when(ahead[1])(functools.partial(near, number))

    def to_later(number):
        for b in others:

            @pl.when(b > me_b)
            def _():
                over(number, b * SPLIT + far_a)
                stay[0](number, b * SPLIT + me_a)

        if number:
            pl.when(jnp.logical_not(ahead[1]))(functools.partial(near, number))

    def to_side(number):
        send_w(0, side_far, w_half(0), w_side)(number, side_c)
        send_v(side_far, v_half, v_side)(number, side_c)
        send_w(0, side_a, w_slot(0, me_c), w_side)(number, side_c)
        send_v(side_a, v_own, v_side)(number, side_c)

    for number in numbers[:-1]:
        to_earlier(number)
    wait_for(entered.at[0], count_of(0, False))
    for number in numbers[:-1]:
        to_side(number)
    wait_for(entered.at[1], count_of(1, False))
    pl.when(jnp.logical_not(ahead[1]))(functools.partial(near, 0))
    wait_for(entered.at[2], count_of(2, False))
    for number in numbers[:-1]:
        to_later(number)
    v_tail[...] = jnp.zeros_like(v_tail)
    w_tail[...] = jnp.zeros_like(w_tail)
    for copy in whole:
        copy.wait()
    if rest:
        edge = (SPLIT - 1) * site + main
        v_tail[:, :rest] = v_all[:, edge:edge + rest]
        w_tail[:, :, :rest] = w_all[:, :, edge:edge + rest]
    for send_last in (to_earlier, to_side, to_later):
        send_last(numbers[-1])
    for number in numbers:
        send_w(1, side_far, w_half(1), w_side)(number, side_c)
        send_w(1, side_a, w_slot(1, me_c), w_side)(number, side_c)

    @pl.when(inner)
    def _():
        for number in numbers:
            for b in others:
                across[1](number, b * SPLIT + far_a)

    for number in numbers:
        start(
            lambda src: pltpu.make_async_copy(src, v_own(number), l_sem.at[0]),
            v_ref, v_tail, me_a, number,
        )
        start(
            lambda src: pltpu.make_async_copy(src, w_s.at[:, me_c, :, cols_of(number)], l_sem.at[1]),
            w_ref, w_tail, me_a, number,
        )

    for number in numbers:
        wait(w_s.at[0, pl.ds(0, 2), :, cols_of(number)], w_side.at[0, number])
        wait(v_s.at[pl.ds(0, 2), :, cols_of(number)], v_side.at[number])
        far(number, stay_on[0], across_on[0])
        near_v_on(number, far_c)
        across_on[0](number, far_c)

    if lent:

        @pl.when(inner)
        def _():
            for number in numbers[:lent]:
                lend = w_slot(0, far_c)(number)
                wait(lend, lend_came.at[0, number])
                for b in others:
                    remote(
                        lend, lend, lend_sent, w_came.at[0, number], me_r, b * SPLIT + me_a
                    ).start()

    for number in numbers[:early]:

        @pl.when(jnp.logical_not(inner))
        def _():
            far(number, stay[1], across[1])

        across[1](number, far_c)
    for number in numbers:
        wait(w_s.at[1, pl.ds(0, 2), :, cols_of(number)], w_side.at[1, number])

        @pl.when(inner)
        def _():
            for b in others:
                across_on[1](number, b * SPLIT + far_a)

        if number < early:

            @pl.when(jnp.logical_not(inner))
            def _():
                far(number, stay_on[1], across_on[1])

            across_on[1](number, far_c)

    @pl.when(inner)
    def _():
        for number in numbers:
            for b in others:
                stay[1](number, b * SPLIT + me_a)
                stay_on[1](number, b * SPLIT + me_a)

    wait_for(entered.at[3], count_of(3, False))
    for k, mask in enumerate(steps):
        _, r, c = partner(mask)
        pl.semaphore_signal(told.at[k], device_id={"prow": r, "pcol": c}, device_id_type=MESH)
        pl.semaphore_wait(told.at[k], 1)

    def panel_of(p, cols):
        block = w_s[p, :, :, cols]
        if w_s.shape[2] % 16:
            block = block.astype(F32)
        return block.reshape(panel, block.shape[-1]).astype(BF16)

    def products(p, at, stop):
        cols = pl.ds(at, stop - at)
        v = v_s[:, :, cols].reshape(rows, stop - at)
        part[...] += lax.dot_general(v, panel_of(p, cols), NT, preferred_element_type=F32)

    def factor_of(p, sums):
        return lax.dot_general(
            sums, t_s[p], NT, precision=lax.Precision.HIGHEST, preferred_element_type=F32
        ).astype(BF16)

    def update(p, at, stop):
        @pl.loop(at // n_block, stop // n_block)
        def _(i):
            cols = pl.ds(pl.multiple_of(i * n_block, n_block), n_block)
            v = v_s[:, :, cols].reshape(rows, n_block).astype(F32)
            v = v - jnp.dot(s_s[...], panel_of(p, cols), preferred_element_type=F32)
            v_s[:, :, cols] = v.astype(BF16).reshape(SPLIT, rows // SPLIT, n_block)

    wait(v_s.at[0, :, pl.ds(0, site)], l_sem.at[0])
    wait(w_s.at[:, 0, :, pl.ds(0, site)], l_sem.at[1])
    for number in numbers:
        wait(v_s.at[pl.ds(0, 2), :, cols_of(number)], v_came.at[number])
        if number < lent:
            for own_role, slots in ((inner, n_col - 3), (jnp.logical_not(inner), n_col - 2)):
                pl.when(own_role)(functools.partial(
                    wait, w_s.at[0, pl.ds(0, slots), :, cols_of(number)], w_came.at[0, number]
                ))
        else:
            wait(w_s.at[0, pl.ds(0, n_col - 2), :, cols_of(number)], w_came.at[0, number])
        products(0, *sums_at[number])

    m_send[...] = part[...].reshape(m_send.shape)
    part[...] = jnp.zeros_like(part)
    for g, r, c in near_by:
        h = lax.rem(g, plane)
        remote(m_send.at[h], m_recv.at[me_h], m_sems.at[0], m_sems.at[1], r, c).start()
    m_recv[me_h] = m_send[me_h]
    wait(m_recv.at[pl.ds(0, plane - 1)], m_sems.at[1])
    z_send[...] = jnp.sum(m_recv[...], axis=0)
    remote(z_send, z_recv, m_sems.at[2], m_sems.at[3], me_r, far_c).start()
    for number in numbers[early:]:

        @pl.when(jnp.logical_not(inner))
        def _():
            far(number, stay[1], across[1])

        across[1](number, far_c)

        @pl.when(jnp.logical_not(inner))
        def _():
            far(number, stay_on[1], across_on[1])

        across_on[1](number, far_c)
    wait(z_recv, m_sems.at[3])
    m_all[me_h] = z_send[...] + z_recv[...]
    for _, r, c in near_by:
        remote(m_all.at[me_h], m_all.at[me_h], m_sems.at[4], m_sems.at[5], r, c).start()
    keep_t.wait()
    wait(m_all.at[pl.ds(0, plane - 1)], m_sems.at[5])
    s_s[...] = factor_of(0, m_all[...].reshape(rows, panel))
    update(0, 0, width)

    for number in numbers:
        wait(w_s.at[1, pl.ds(0, n_col - 2), :, cols_of(number)], w_came.at[1, number])
        products(1, *sums_at[number])

    rs_send[...] = part[...].astype(BF16).reshape(rs_send.shape)
    for g, r, c in partners:
        remote(rs_send.at[g], rs_recv.at[me_g], r_send, r_recv, r, c).start()
    rs_recv[me_g] = rs_send[me_g]
    wait(rs_recv.at[pl.ds(0, group - 1)], r_recv)
    ag[me_g] = factor_of(1, jnp.sum(rs_recv[...].astype(F32), axis=0))
    for g, r, c in partners:
        remote(ag.at[me_g], ag.at[me_g], g_send, g_recv, r, c).start()
    wait(ag.at[pl.ds(0, group - 1)], g_recv)
    s_s[...] = ag[...].reshape(rows, panel)

    def rows_of(r):
        return pl.ds(pl.multiple_of(r * own, own), own)

    for j, (at, stop) in enumerate(out_blocks):
        update(1, at, stop)
        cols = pl.ds(at, min(stop, site) - at)
        for g, r, c in partners:
            remote(
                v_s.at[lax.div(g, n_row), rows_of(r), cols], stage.at[me_g, :, cols],
                o_send, o_recv.at[j], r, c,
            ).start()

    for j, (at, stop) in enumerate(out_blocks):
        size = min(stop, site) - at
        cols = pl.ds(at, size)
        stage[me_g, :, cols] = v_s[me_a, rows_of(me_r), cols]
        wait(stage.at[pl.ds(0, group - 1), :, cols], o_recv.at[j])
        for r in range(n_row):
            for a in range(SPLIT):
                size = min(at + size, columns - a * site) - at
                begin = r * columns + a * site + at
                if size > 0:
                    o_ref[:, begin:begin + size] = stage[a * n_row + r, :, at:at + size]
                size = min(stop, site) - at
    wait(v_s.at[:, :, pl.ds(0, site)], v_sent)
    cut = pieces[lent][0]
    wait(w_s.at[1, :, :, pl.ds(0, site)], w_sent.at[0])
    if lent:
        wait(w_s.at[0, pl.ds(0, n_col - len(others)), :, pl.ds(0, cut)], w_sent.at[1])

        @pl.when(inner)
        def _():
            wait(w_s.at[0, pl.ds(0, 2 * len(others)), :, pl.ds(0, cut)], lend_sent)

    wait(w_s.at[0, :, :, pl.ds(cut, site - cut)], w_sent.at[2])
    wait(m_recv.at[pl.ds(0, plane - 1)], m_sems.at[0])
    wait(z_send, m_sems.at[2])
    wait(m_all.at[pl.ds(0, plane - 1)], m_sems.at[4])
    wait(rs_recv.at[pl.ds(0, group - 1)], r_send)
    wait(ag.at[pl.ds(0, group - 1)], g_send)
    wait(stage.at[pl.ds(0, group - 1)], o_send)


def body(n_row, n_col, vectors, reflectors, panel_factor):
    own_rows, columns = vectors.shape
    part_rows, panel = reflectors.shape[1], panel_factor.shape[1]
    group, plane, rows = SPLIT * n_row, 2 * n_row, SPLIT * own_rows
    site = -(-columns // (SPLIT * LANES)) * LANES
    last = columns - (SPLIT - 1) * site
    main, rest = last // LANES * LANES, last % LANES
    n_block = 2 * LANES
    width = -(-site // n_block) * n_block
    step = -(-main // (4 * n_block)) * n_block
    cuts = list(range(0, main, step)) + [main]
    even = main // n_block * n_block
    pieces = tuple(zip(cuts[:-1], cuts[1:])) + ((main, site),)
    sums_at = tuple((s, min(e, even)) for s, e in pieces[:-1]) + ((even, width),)
    marks = [0, n_block]
    blocks = width // n_block
    marks += [n_block * (1 + (blocks - 1) * k // 6) for k in range(1, 7)]
    out_blocks = tuple(zip(marks[:-1], marks[1:]))
    count = len(pieces)
    dma = pltpu.SemaphoreType.DMA
    plan = (site, main, rest, pieces, sums_at, out_blocks, n_block, 2, 2)
    whole = pl.pallas_call(
        functools.partial(kernel, n_row, n_col, columns, plan),
        out_shape=jax.ShapeDtypeStruct((own_rows // n_row, n_row * columns), BF16),
        in_specs=[
            pl.BlockSpec(memory_space=pl.ANY),
            pl.BlockSpec(memory_space=pl.ANY),
            pl.BlockSpec(memory_space=pltpu.HBM),
        ],
        out_specs=pl.BlockSpec(memory_space=pltpu.VMEM),
        scratch_shapes=[
            pltpu.VMEM((SPLIT, own_rows, width), BF16),
            pltpu.VMEM((2, n_col, part_rows, width), BF16),
            pltpu.VMEM((own_rows, site), BF16),
            pltpu.VMEM((2, part_rows, site), BF16),
            pltpu.VMEM((own_rows, site - main), BF16),
            pltpu.VMEM((2, part_rows, site - main), BF16),
            pltpu.VMEM(vectors.shape, BF16),
            pltpu.VMEM(reflectors.shape, BF16),
            pltpu.VMEM(panel_factor.shape, F32),
            pltpu.VMEM((rows, panel), F32),
            pltpu.VMEM((rows, panel), BF16),
            pltpu.VMEM((group, own_rows // n_row, site), BF16),
            pltpu.VMEM((plane, rows // plane, panel), F32),
            pltpu.VMEM((plane, rows // plane, panel), F32),
            pltpu.VMEM((rows // plane, panel), F32),
            pltpu.VMEM((rows // plane, panel), F32),
            pltpu.VMEM((plane, rows // plane, panel), F32),
            pltpu.VMEM((group, rows // group, panel), BF16),
            pltpu.VMEM((group, rows // group, panel), BF16),
            pltpu.VMEM((group, rows // group, panel), BF16),
            dma, dma((3,)), dma((count,)), dma((2, count)), dma((count,)), dma((2, count)), dma((2,)), dma((3,)),
            dma, dma((1, count)),
            dma((6,)), dma, dma, dma, dma, dma, dma((len(out_blocks),)),
            pltpu.SemaphoreType.REGULAR((4,)),
            pltpu.SemaphoreType.REGULAR((group.bit_length() - 1,)),
        ],
        compiler_params=pltpu.CompilerParams(
            has_side_effects=True, collective_id=0, vmem_limit_bytes=48 * 1024 * 1024
        ),
        name="panels",
    )(
        vectors, reflectors,
        pltpu.with_memory_space_constraint(panel_factor, pltpu.HBM),
    )
    return whole[None]


def solution(mesh):
    placed = (P("pcol", "prow"), P(None, "pcol", "prow"), P())
    return jax.shard_map(
        functools.partial(body, mesh.shape["prow"], mesh.shape["pcol"]),
        mesh=mesh, in_specs=placed, out_specs=P("pcol", "prow", None), check_vma=False,
    )
```
